128 devices in a mesh: gx: 8 (over z_lo, y), gy: 16 (over z_hi, x, core).
Axes of the slice: x: 4, y: 4, z: 4 (z_hi: 2, z_lo: 2; z = z_hi * 2 + z_lo), core: 2. Of those that a mesh axis runs over, the one named last changes fastest.
Arguments:
- u_wind: float32 [60, 512, 2048], P(None, 'gx', 'gy'), may hold values from -6 to 6
- v_wind: float32 [60, 512, 2048], P(None, 'gx', 'gy'), may hold values from -6 to 6
- w_wind: float32 [60, 512, 2048], P(None, 'gx', 'gy'), may hold values from -3 to 3
- pressure: float32 [60, 512, 2048], P(None, 'gx', 'gy'), may hold values from -6 to 6
- vert_coef: float32 [512, 2048], P('gx', 'gy'), may hold values from 0.2 to 5
- we_slab: float32 [2, 3, 60, 5, 2048], P(None, None, None, None, ('gy', 'gx')), may hold values from -8 to 8
- sn_slab: float32 [2, 3, 60, 5, 512], P(None, None, None, None, ('gx', 'gy')), may hold values from -8 to 8
- relax_width: int32 [512, 2048], P('gx', 'gy'), may hold values from 2 to 5
Outputs:
- u_out: float32 [60, 512, 2048], P(None, 'gx', 'gy')
- v_out: float32 [60, 512, 2048], P(None, 'gx', 'gy')
- w_out: float32 [60, 512, 2048], P(None, 'gx', 'gy')
- p_out: float32 [60, 512, 2048], P(None, 'gx', 'gy')
The draws below stay inside these ranges and needn't reach their ends.
All inputs are finite; a program needn't handle non-finite values.
Results may differ from the reference program's by a relative error of at most 0.0001.
Values sent between devices are 32-bit elements; how exact they have to be, the bound alone decides.
No kernel may reach another device: no remote copies, remote signals or barrier semaphores. Data moves between devices by JAX's collectives and lax.ppermute only.
A program may use at most 192 MiB of HBM per device.

```python
import math
import jax
import jax.numpy as jnp
from jax import lax

NZ = 60
W = 5
SUBSTEPS = 6
NX = 512
NY = 2048


def place_ends(drawn, stream_key, smallest, largest):
    shape = drawn.shape
    place = [jax.random.randint(jax.random.fold_in(stream_key, axis), (), 0, shape[axis]) for axis in range(len(shape))]
    drawn = drawn.at[tuple(place)].set(smallest)
    longest = shape.index(max(shape))
    place[longest] = (place[longest] + 1) % shape[longest]
    return drawn.at[tuple(place)].set(largest)


def level_of(rng, shape, split, smallest, high):
    level = 1.0
    for position, blocks in split:
        draws = jax.random.uniform(jax.random.fold_in(jax.random.fold_in(rng, 6), position), (blocks,), jnp.float32, smallest / len(split), high / len(split))
        level = level * jnp.repeat(jnp.exp(draws), shape[position] // blocks).reshape((-1,) + (1,) * (len(shape) - 1 - position))
    return level


def normal_values(own_key, dims, deviation, bound, pieces=(), kind=jnp.bfloat16):
    array = deviation * jax.random.normal(own_key, dims, jnp.float32)
    if pieces:
        array = array * level_of(own_key, dims, pieces, -0.22, 0.18)
    return jnp.clip(array, -bound, bound).astype(kind)


def setup_inputs(seed: int = 0) -> dict:
    seeds = jax.random.split(jax.random.key(seed), 9)
    u_wind = normal_values(seeds[0], (NZ, NX, NY), 1.0, 6.0, ((1, 8), (2, 16)), jnp.float32)
    v_wind = normal_values(seeds[1], (NZ, NX, NY), 1.0, 6.0, ((1, 8), (2, 16)), jnp.float32)
    w_wind = normal_values(seeds[2], (NZ, NX, NY), 0.5, 3.0, ((1, 8), (2, 16)), jnp.float32)
    pressure = normal_values(seeds[3], (NZ, NX, NY), 1.0, 6.0, ((1, 8), (2, 16)), jnp.float32)
    vert_coef = jnp.clip(jnp.exp(math.log(5.0) - 3.218876 * jax.random.uniform(seeds[4], (NX, NY), jnp.float32) ** level_of(seeds[4], (NX, NY), ((0, 8), (1, 16)), -0.2, 0.2)), 0.2, 5.0)
    we_slab = normal_values(seeds[5], (2, 3, NZ, W, NY), 1.5, 8.0, ((4, 128),), jnp.float32)
    sn_slab = normal_values(seeds[6], (2, 3, NZ, W, NX), 1.5, 8.0, ((4, 128),), jnp.float32)
    relax_width = place_ends(jax.random.randint(seeds[7], (NX, NY), 2, W + 1), jax.random.fold_in(seeds[7], 1), 2, W).astype(jnp.int32)
    return dict(u_wind=u_wind, v_wind=v_wind, w_wind=w_wind, pressure=pressure, vert_coef=vert_coef, we_slab=we_slab, sn_slab=sn_slab, relax_width=relax_width)


accel = 0.3
spread = 0.3
buoyancy = 0.5


def tri_solve(coef, rhs):
    def forward(carry, item):
        prev_c, prev_d = carry
        denom = 1.0 + 2.0 * coef + coef * prev_c
        next_c = -coef / denom
        next_d = (item + coef * prev_d) / denom
        return (next_c, next_d), (next_c, next_d)

    zero = jnp.zeros_like(coef)
    _, (cees, dees) = lax.scan(forward, (zero, zero), rhs)

    def backward(above, item):
        c_here, d_here = item
        value = d_here - c_here * above
        return value, value

    _, solved = lax.scan(backward, zero, (cees, dees), reverse=True)
    return solved


def blend(field, rows_k, cols_k, xpos, ypos, nx_total, ny_total, rate):
    band = rows_k.shape[2]
    size_x = field.shape[1]
    size_y = field.shape[2]
    west = jnp.pad(rows_k[0], ((0, 0), (0, size_x - band), (0, 0)))
    east = jnp.pad(rows_k[1][:, ::-1, :], ((0, 0), (size_x - band, 0), (0, 0)))
    south = jnp.pad(jnp.transpose(cols_k[0], (0, 2, 1)), ((0, 0), (0, 0), (0, size_y - band)))
    north = jnp.pad(jnp.transpose(cols_k[1][:, ::-1, :], (0, 2, 1)), ((0, 0), (0, 0), (size_y - band, 0)))
    weight_w = jnp.maximum(rate - xpos[:, None], 0.0) / rate
    weight_e = jnp.maximum(rate - (nx_total - 1.0 - xpos)[:, None], 0.0) / rate
    weight_s = jnp.maximum(rate - ypos[None, :], 0.0) / rate
    weight_n = jnp.maximum(rate - (ny_total - 1.0 - ypos)[None, :], 0.0) / rate
    field = field + weight_w[None] * (west - field)
    field = field + weight_e[None] * (east - field)
    field = field + weight_s[None] * (south - field)
    field = field + weight_n[None] * (north - field)
    return field


def column_part(u_new, v_new, west_u, south_v, w_old, p_old, coef):
    diverge = (u_new - west_u) + (v_new - south_v)
    sectioned = p_old - spread * diverge
    above_q = jnp.concatenate([sectioned[1:], jnp.zeros_like(sectioned[:1])], axis=0)
    rhs = w_old + buoyancy * (sectioned - above_q)
    w_new = tri_solve(coef, rhs)
    below_w = jnp.concatenate([jnp.zeros_like(w_new[:1]), w_new[:-1]], axis=0)
    p_new = sectioned - buoyancy * (w_new - below_w)
    return w_new, p_new


def reference(u_wind, v_wind, w_wind, pressure, vert_coef, we_slab, sn_slab, relax_width):
    size_x = pressure.shape[1]
    size_y = pressure.shape[2]
    xpos = jnp.arange(size_x, dtype=jnp.int32).astype(jnp.float32)
    ypos = jnp.arange(size_y, dtype=jnp.int32).astype(jnp.float32)
    rate = relax_width.astype(jnp.float32)
    fields = []
    for index, field in enumerate((u_wind, v_wind, pressure)):
        fields.append(blend(field, we_slab[:, index], sn_slab[:, index], xpos, ypos, float(size_x), float(size_y), rate))
    u_now, v_now, p_now = fields
    w_now = w_wind
    for step in range(SUBSTEPS):
        east_p = jnp.concatenate([p_now[:, 1:, :], jnp.zeros_like(p_now[:, :1, :])], axis=1)
        north_p = jnp.concatenate([p_now[:, :, 1:], jnp.zeros_like(p_now[:, :, :1])], axis=2)
        u_now = u_now - accel * (east_p - p_now)
        v_now = v_now - accel * (north_p - p_now)
        west_u = jnp.concatenate([jnp.zeros_like(u_now[:, :1, :]), u_now[:, :-1, :]], axis=1)
        south_v = jnp.concatenate([jnp.zeros_like(v_now[:, :, :1]), v_now[:, :, :-1]], axis=2)
        w_now, p_now = column_part(u_now, v_now, west_u, south_v, w_now, p_now, vert_coef)
    return u_now, v_now, w_now, p_now
```

```python
import jax
import jax.numpy as jnp
from jax import lax
from jax.experimental import pallas as pl
from jax.experimental.pallas import tpu as pltpu
from jax.sharding import PartitionSpec as P

SUBSTEPS = 6
HALO = 6
OFF = 16
ZG = 6
LANES = 128
ACCEL = 0.3
SPREAD = 0.3
SROW = 8
NROW = 32
SROWS = 56

VMEM = pl.BlockSpec(memory_space=pltpu.VMEM)


def passed_along(block, axis, distance):
    devices = range(lax.axis_size(axis))
    route = [(i - distance, i) for i in devices if i - distance in devices]
    return lax.ppermute(block, axis, route)


def lane_pairs(bands):
    levels = bands.shape[-1]
    low = jnp.pad(bands[:8], ((0, 0), (0, 0), (0, LANES - levels)))
    high = jnp.pad(bands[8:], ((0, 1), (0, 0), (64, 64 - levels)))
    return low + high


def to_edges(slab, axis):
    size = lax.axis_size(axis)
    t = jnp.transpose(slab, (0, 1, 3, 4, 2))
    first = lane_pairs(t[0].reshape(15, *t.shape[3:]))
    last = lane_pairs(t[1, :, ::-1].reshape(15, *t.shape[3:]))
    zero = jnp.zeros((size - 2, *first.shape), first.dtype)
    sent = jnp.concatenate([first[None], zero, last[None]], axis=0)
    return lax.all_to_all(sent, axis, 0, 0, tiled=True)


def iota8(dim):
    return lax.broadcasted_iota(jnp.int32, (8, LANES), dim)


def blend_kernel(nx, ny, u, v, p, w, coef, width, weg, sng, ub, vb, pb, east, west, cw, ce, bs, bt, wsn):
    levels, size_x, _ = u.shape
    gx = lax.axis_index("gx")
    gy = lax.axis_index("gy")
    blocks = size_x // 8
    groups = weg.shape[0]
    zero = jnp.zeros((8, LANES), jnp.float32)

    def clear(i, _):
        for k in range(3):
            cw[k, pl.ds(pl.multiple_of(i * 8, 8), 8), :] = zero
            ce[k, pl.ds(pl.multiple_of(i * 8, 8), 8), :] = zero
            bs[k, pl.ds(pl.multiple_of(i * 8, 8), 8), :] = zero
        return 0

    lax.fori_loop(0, 64, clear, 0)
    for s in range(8):
        a = jnp.concatenate([weg[g, s] for g in range(groups)], axis=0).T
        b = jnp.concatenate([sng[s], jnp.zeros((LANES - size_x, LANES), jnp.float32)], axis=0).T
        for half in range(2):
            kj = s + 8 * half
            if kj < 15:
                k, j = kj // 5, kj % 5
                cw[k, pl.ds(j, 64, stride=8), :] = a[64 * half : 64 * half + 64]
                ce[k, pl.ds(3 + j, 64, stride=8), :] = a[64 * half : 64 * half + 64]
                bs[k, pl.ds(j, 64, stride=8), :] = b[64 * half : 64 * half + 64]
    for k in range(3):
        for g in range(4):
            bt[k, g] = bs[k, g * LANES : (g + 1) * LANES, :].T

    sub = iota8(0).astype(jnp.float32)
    lane = iota8(1).astype(jnp.float32)
    x0 = (gx * size_x).astype(jnp.float32)
    y0 = (gy * LANES).astype(jnp.float32)
    is_north = gy == lax.axis_size("gy") - 1
    rate_w = width[0:8, :].astype(jnp.float32)
    rate_e = width[size_x - 8 : size_x, :].astype(jnp.float32)
    weight_w = jnp.maximum(rate_w - (sub + x0), 0.0) / rate_w
    dist_e = (nx - 1.0) - (sub + (x0 + (size_x - 8.0)))
    weight_e = jnp.maximum(rate_e - dist_e, 0.0) / rate_e

    fields = ((p, pb, 2), (u, ub, 0), (v, vb, 1))

    def take(z, _):
        rows = pl.ds(pl.multiple_of(z * 8, 8), 8)
        for src, dst, k in fields:
            for b in range(blocks):
                val = src[z, 8 * b : 8 * b + 8, :]
                if b == 0:
                    val = val + weight_w * (cw[k, rows, :] - val)
                if b == blocks - 1:
                    val = val + weight_e * (ce[k, rows, :] - val)
                dst[z, 8 * b : 8 * b + 8, :] = val
        return 0

    lax.fori_loop(0, levels, take, 0)

    @pl.when((gy == 0) | is_north)
    def _():
        dist = jnp.where(is_north, (ny - 1.0) - (lane + y0), lane + y0)
        for b in range(blocks):
            rate = width[8 * b : 8 * b + 8, :].astype(jnp.float32)
            wsn[8 * b : 8 * b + 8, :] = jnp.maximum(rate - dist, 0.0) / rate
        base = jnp.where(is_north, 123 + LANES, LANES)

        def sides(z, _):
            g = z // 16
            shift = lax.rem(base - 8 * lax.rem(z, 16), LANES)
            for _, dst, k in fields:
                for b in range(blocks):
                    band = pltpu.roll(bt[k, g, 8 * b : 8 * b + 8, :], shift, 1)
                    val = dst[z, 8 * b : 8 * b + 8, :]
                    dst[z, 8 * b : 8 * b + 8, :] = val + wsn[8 * b : 8 * b + 8, :] * (band - val)
            return 0

        lax.fori_loop(0, levels, sides, 0)

    def pack(z, _):
        for f, src in enumerate((pb, ub, vb, w)):
            east[z, HALO * f : HALO * f + HALO, :] = src[z, size_x - HALO : size_x, :]
            west[z, HALO * f : HALO * f + HALO, :] = src[z, 0:HALO, :]
        return 0

    lax.fori_loop(0, levels, pack, 0)
    for msg, lo in ((east, size_x - HALO), (west, 0)):
        for b in range(3):
            msg[levels, 8 * b : 8 * b + 8, :] = zero
        msg[levels, 0:HALO, :] = coef[lo : lo + HALO, :]


def strip_kernel(p, u, v, w, coef, from_w, from_e, own, own_r, north, south, halo):
    levels, size_x, _ = u.shape
    blocks = size_x // 8
    zero = jnp.zeros((8, LANES), jnp.float32)
    lane_group = iota8(1) // 16

    def unpack(z, _):
        for f in range(4):
            halo[f, z, 0:8, :] = zero
            halo[f, z, 8:16, :] = zero
            halo[f, z, 2:8, :] = from_w[z, HALO * f : HALO * f + HALO, :]
            halo[f, z, 8:14, :] = from_e[z, HALO * f : HALO * f + HALO, :]
        return 0

    lax.fori_loop(0, levels + 1, unpack, 0)

    def turned(parts):
        rows = [zero] + parts + [zero] * (LANES // 8 - 1 - len(parts))
        return jnp.concatenate(rows, axis=0).T

    for f, src in enumerate((p, u, v, w)):

        def group(g, _):
            acc = None
            for zi in range(ZG):
                z = g * ZG + zi
                parts = [halo[f, z, 0:8, :]]
                parts += [src[z, 8 * b : 8 * b + 8, :] for b in range(blocks)]
                parts += [halo[f, z, 8:16, :]]
                parts = [pltpu.roll(part, (8 + 16 * zi) % LANES, 1) for part in parts]
                if acc is None:
                    acc = parts
                else:
                    acc = [jnp.where(lane_group == zi, part, old) for part, old in zip(parts, acc)]
            t = turned(acc)
            for zi in range(ZG):
                z = g * ZG + zi
                both = t[16 * zi : 16 * zi + 16]
                own[f, z] = both
                north[z, HALO * f : HALO * f + HALO, :] = both[2:8]
                south[z, HALO * f : HALO * f + HALO, :] = both[8:14]
            return 0

        lax.fori_loop(0, levels // ZG, group, 0)

    parts = [halo[0, levels, 0:8, :]]
    parts += [coef[8 * b : 8 * b + 8, :] for b in range(blocks)]
    parts += [halo[0, levels, 8:16, :]]
    t = turned([pltpu.roll(part, 8, 1) for part in parts])
    own_r[...] = t[0:16]
    for msg in (north, south):
        for b in range(3):
            msg[levels, 8 * b : 8 * b + 8, :] = zero
    north[levels, 0:HALO, :] = t[2:8]
    south[levels, 0:HALO, :] = t[8:14]


def step_kernel(
    ub, vb, pb, w_in, coef, from_w, from_e, own, own_r, from_s, from_n,
    u_out, v_out, w_out, p_out,
    P_, E_, W_, S_, M_, R_, sP, sE, sW, sU, sM, sR, rows, T_,
):
    levels, size_x, _ = ub.shape
    blocks = size_x // 8
    starts = [8 * b for b in range(1, blocks + 3)]
    main = [OFF + 8 * b for b in range(blocks)]
    sstarts = [SROW, SROW + 8, NROW, NROW + 8]
    zero = jnp.zeros((8, LANES), jnp.float32)
    sub = iota8(0)
    lane = iota8(1)
    is_west = lax.axis_index("gx") == 0
    is_east = lax.axis_index("gx") == lax.axis_size("gx") - 1
    is_south = lax.axis_index("gy") == 0
    is_north = lax.axis_index("gy") == lax.axis_size("gy") - 1
    mask_w = (sub == 0) & is_west
    mask_e = (sub == 7) & is_east
    smask_w = (lane == OFF) & is_west
    smask_e = (lane == OFF + size_x - 1) & is_east
    smask_s = (sub == 0) & is_south
    smask_n = (sub == 7) & is_north
    lane0 = lane == 0
    lane127 = lane == LANES - 1
    AB = ACCEL * SPREAD

    def unpack(z, _):
        for f, src, dst, sdst in ((0, pb, P_, sP), (1, ub, S_, sU), (2, vb, M_, sM), (3, w_in, W_, sW)):
            scale = 2.0 if f == 3 else 1.0
            for r in (0, 8, OFF + size_x, OFF + size_x + 8):
                dst[z, r : r + 8, :] = zero
            for b in range(blocks):
                dst[z, OFF + 8 * b : OFF + 8 * b + 8, :] = src[z, 8 * b : 8 * b + 8, :] * scale
            lo = HALO * f
            dst[z, OFF - HALO : OFF, :] = from_w[z, lo : lo + HALO, :] * scale
            dst[z, OFF + size_x : OFF + size_x + HALO, :] = from_e[z, lo : lo + HALO, :] * scale
            for r in range(0, SROWS, 8):
                sdst[z, r : r + 8, :] = zero
            sdst[z, SROW + 8 : SROW + 16, :] = own[f, z, 8:16, :] * scale
            sdst[z, NROW : NROW + 8, :] = own[f, z, 0:8, :] * scale
            sdst[z, SROW + 8 - HALO : SROW + 8, :] = from_s[z, lo : lo + HALO, :] * scale
            sdst[z, NROW + 8 : NROW + 8 + HALO, :] = from_n[z, lo : lo + HALO, :] * scale
        return 0

    lax.fori_loop(0, levels, unpack, 0)
    R_[...] = jnp.zeros_like(R_)
    R_[OFF : OFF + size_x, :] = coef[...]
    R_[OFF - HALO : OFF, :] = from_w[levels, 0:HALO, :]
    R_[OFF + size_x : OFF + size_x + HALO, :] = from_e[levels, 0:HALO, :]
    sR[...] = jnp.zeros_like(sR)
    sR[SROW + 8 : SROW + 16, :] = own_r[8:16, :]
    sR[NROW : NROW + 8, :] = own_r[0:8, :]
    sR[SROW + 8 - HALO : SROW + 8, :] = from_s[levels, 0:HALO, :]
    sR[NROW + 8 : NROW + 8 + HALO, :] = from_n[levels, 0:HALO, :]
    rows[...] = jnp.zeros_like(rows)

    def strip_init(z, _):
        for s in sstarts:
            u = sU[z, s : s + 8, :]
            v = sM[z, s : s + 8, :]
            v_s = sM[z, s - 1 : s + 7, :]
            sE[z, s : s + 8, :] = SPREAD * ((u - pltpu.roll(u, 1, 1)) + (v - v_s))
        rows[SUBSTEPS, pl.ds(2 * z, 1), :] = sM[z, SROW + 7 : SROW + 8, :]
        return 0

    lax.fori_loop(0, levels, strip_init, 0)

    def factors(coefs, dst, at):
        def body(z, prev):
            new = []
            for s, m in zip(at, prev):
                r = coefs[s : s + 8, :]
                m = 1.0 / (1.0 + 2.0 * r - r * r * m)
                dst[z, s : s + 8, :] = m
                new.append(m)
            return tuple(new)

        lax.fori_loop(0, levels, body, tuple(zero for _ in at))

    factors(sR, sM, sstarts)

    def substep(pp, ww, mm, rr, at, sectioned):
        def store(z, qs):
            for s, q in zip(at, qs):
                pp[z, s : s + 8, :] = q

        def down(z, qs, qn, ds):
            new = []
            for i, s in enumerate(at):
                rhs = ww[z, s : s + 8, :] + (qs[i] if qn is None else qs[i] - qn[i])
                if ds is not None:
                    rhs = rhs + rr[s : s + 8, :] * ds[i]
                d = mm[z, s : s + 8, :] * rhs
                ww[z, s : s + 8, :] = d
                new.append(d)
            return tuple(new)

        qs = sectioned(0)
        store(0, qs)

        def fwd(z, carry):
            qs, ds = carry
            qn = sectioned(z)
            store(z, qn)
            return qn, down(z - 1, qs, qn, ds)

        qs, ds = lax.fori_loop(1, levels, fwd, (qs, tuple(zero for _ in at)))
        ws = down(levels - 1, qs, None, ds)

        def bwd(i, ws):
            z = levels - 2 - i
            new = []
            for j, s in enumerate(at):
                w = ww[z, s : s + 8, :] + mm[z, s : s + 8, :] * (rr[s : s + 8, :] * ws[j])
                ww[z, s : s + 8, :] = w
                pp[z + 1, s : s + 8, :] = pp[z + 1, s : s + 8, :] - 0.25 * (ws[j] - w)
                new.append(w)
            return tuple(new)

        ws = lax.fori_loop(0, levels - 1, bwd, ws)
        for j, s in enumerate(at):
            pp[0, s : s + 8, :] = pp[0, s : s + 8, :] - 0.25 * ws[j]

    def strip_step(k, _):
        def sectioned(z):
            qs = []
            for s in sstarts:
                p = sP[z, s : s + 8, :]
                p_s = sP[z, s - 1 : s + 7, :]
                p_n = sP[z, s + 1 : s + 9, :]
                p_w = jnp.where(smask_w, p, pltpu.roll(p, 1, 1))
                p_e = jnp.where(smask_e, 0.0, pltpu.roll(p, LANES - 1, 1))
                if s == SROW + 8:
                    p_s = jnp.where(smask_s, p, p_s)
                if s == NROW:
                    p_n = jnp.where(smask_n, 0.0, p_n)
                e = sE[z, s : s + 8, :] - AB * (((p_w + p_e) + (p_s + p_n)) - 4.0 * p)
                sE[z, s : s + 8, :] = e
                qs.append(p - e)
            edge_s = jnp.where(is_south, sP[z, SROW + 8 : SROW + 9, :], sP[z, SROW + 7 : SROW + 8, :])
            edge_n = jnp.where(is_north, 0.0, sP[z, NROW + 8 : NROW + 9, :])
            rows[k, pl.ds(2 * z, 1), :] = edge_s
            rows[k, pl.ds(lax.rem(2 * z + LANES - 1, LANES), 1), :] = edge_n
            return tuple(qs)

        substep(sP, sW, sM, sR, sstarts, sectioned)
        return 0

    lax.fori_loop(0, SUBSTEPS, strip_step, 0)

    for k in range(SUBSTEPS + 1):
        T_[k] = rows[k].T

    def edges(k, z, s):
        return pltpu.roll(T_[k, s : s + 8, :], lax.rem(2 * LANES - 2 * z, LANES), 1)

    def main_init(z, _):
        for s in starts:
            u = S_[z, s : s + 8, :]
            u_w = S_[z, s - 1 : s + 7, :]
            v = M_[z, s : s + 8, :]
            v_s = jnp.where(lane0, edges(SUBSTEPS, z, s), pltpu.roll(v, 1, 1))
            E_[z, s : s + 8, :] = SPREAD * ((u - u_w) + (v - v_s))
        for s in starts:
            S_[z, s : s + 8, :] = zero
        return 0

    lax.fori_loop(0, levels, main_init, 0)
    factors(R_, M_, starts)

    def main_step(k, _):
        def sectioned(z):
            qs = []
            for s in starts:
                p = P_[z, s : s + 8, :]
                p_w = P_[z, s - 1 : s + 7, :]
                p_e = P_[z, s + 1 : s + 9, :]
                if s == main[0]:
                    p_w = jnp.where(mask_w, p, p_w)
                if s == main[-1]:
                    p_e = jnp.where(mask_e, 0.0, p_e)
                edge = edges(k, z, s)
                p_s = jnp.where(lane0, edge, pltpu.roll(p, 1, 1))
                p_n = jnp.where(lane127, edge, pltpu.roll(p, LANES - 1, 1))
                e = E_[z, s : s + 8, :] - AB * (((p_w + p_e) + (p_s + p_n)) - 4.0 * p)
                E_[z, s : s + 8, :] = e
                S_[z, s : s + 8, :] = S_[z, s : s + 8, :] + p
                qs.append(p - e)
            return tuple(qs)

        substep(P_, W_, M_, R_, starts, sectioned)
        return 0

    lax.fori_loop(0, SUBSTEPS, main_step, 0)

    total = T_[0]
    for k in range(1, SUBSTEPS):
        total = total + T_[k]
    T_[0] = total

    def finish(z, _):
        for b, s in enumerate(main):
            at = slice(8 * b, 8 * b + 8)
            total = S_[z, s : s + 8, :]
            east = S_[z, s + 1 : s + 9, :]
            if s == main[-1]:
                east = jnp.where(mask_e, 0.0, east)
            north = jnp.where(lane127, edges(0, z, s), pltpu.roll(total, LANES - 1, 1))
            u_out[z, at, :] = ub[z, at, :] - ACCEL * (east - total)
            v_out[z, at, :] = vb[z, at, :] - ACCEL * (north - total)
            w_out[z, at, :] = 0.5 * W_[z, s : s + 8, :]
            p_out[z, at, :] = P_[z, s : s + 8, :]
        return 0

    lax.fori_loop(0, levels, finish, 0)


def per_device(u_wind, v_wind, w_wind, pressure, vert_coef, we_slab, sn_slab, relax_width):
    levels, size_x, size_y = pressure.shape
    nx = float(size_x * lax.axis_size("gx"))
    ny = float(size_y * lax.axis_size("gy"))
    weg = to_edges(we_slab, "gx")
    sng = to_edges(sn_slab, "gy")
    sng = jnp.transpose(sng, (1, 0, 2, 3)).reshape(8, size_x, LANES)
    f32 = jnp.float32
    block = jax.ShapeDtypeStruct(pressure.shape, f32)
    message = jax.ShapeDtypeStruct((levels + 1, 4 * HALO, LANES), f32)
    ext = size_x + 2 * OFF

    def kernel(*args):
        blend_kernel(nx, ny, *args)

    ub, vb, pb, east, west = pl.pallas_call(
        kernel,
        out_shape=(block, block, block, message, message),
        in_specs=[VMEM] * 8,
        out_specs=[VMEM] * 5,
        scratch_shapes=[
            pltpu.VMEM((3, 512, LANES), f32),
            pltpu.VMEM((3, 512, LANES), f32),
            pltpu.VMEM((3, 512, LANES), f32),
            pltpu.VMEM((3, 4, LANES, LANES), f32),
            pltpu.VMEM((size_x, LANES), f32),
        ],
        compiler_params=pltpu.CompilerParams(vmem_limit_bytes=30 << 20),
        name="blend",
    )(u_wind, v_wind, pressure, w_wind, vert_coef, relax_width, weg, sng)
    from_w = passed_along(east, "gx", 1)
    from_e = passed_along(west, "gx", -1)

    own, own_r, north, south = pl.pallas_call(
        strip_kernel,
        out_shape=(
            jax.ShapeDtypeStruct((4, levels, 16, LANES), f32),
            jax.ShapeDtypeStruct((16, LANES), f32),
            message,
            message,
        ),
        in_specs=[VMEM] * 7,
        out_specs=[VMEM] * 4,
        scratch_shapes=[pltpu.VMEM((4, levels + 1, 16, LANES), f32)],
        compiler_params=pltpu.CompilerParams(vmem_limit_bytes=30 << 20),
        name="strips",
    )(pb, ub, vb, w_wind, vert_coef, from_w, from_e)
    from_s = passed_along(north, "gy", 1)
    from_n = passed_along(south, "gy", -1)

    big = pltpu.VMEM((levels, ext, LANES), f32)
    strip = pltpu.VMEM((levels, SROWS, LANES), f32)
    return pl.pallas_call(
        step_kernel,
        out_shape=(block, block, block, block),
        in_specs=[VMEM] * 11,
        out_specs=[VMEM] * 4,
        scratch_shapes=[big] * 5
        + [pltpu.VMEM((ext, LANES), f32)]
        + [strip] * 5
        + [
            pltpu.VMEM((SROWS, LANES), f32),
            pltpu.VMEM((SUBSTEPS + 1, LANES, LANES), f32),
            pltpu.VMEM((SUBSTEPS + 1, LANES, LANES), f32),
        ],
        compiler_params=pltpu.CompilerParams(vmem_limit_bytes=56 << 20),
        name="substeps",
    )(ub, vb, pb, w_wind, vert_coef, from_w, from_e, own, own_r, from_s, from_n)


def solution(mesh):
    placed = (
        P(None, "gx", "gy"),
        P(None, "gx", "gy"),
        P(None, "gx", "gy"),
        P(None, "gx", "gy"),
        P("gx", "gy"),
        P(None, None, None, None, ("gy", "gx")),
        P(None, None, None, None, ("gx", "gy")),
        P("gx", "gy"),
    )
    return jax.shard_map(
        per_device,
        mesh=mesh,
        in_specs=placed,
        out_specs=(P(None, "gx", "gy"),) * 4,
        check_vma=False,
    )
```

```python
import jax
import jax.numpy as jnp
from jax import lax
from jax.experimental import pallas as pl
from jax.experimental.pallas import tpu as pltpu
from jax.sharding import PartitionSpec as P

SUBSTEPS = 6
HALO = 6
OFF = 16
ZG = 6
LANES = 128
ACCEL = 0.3
SPREAD = 0.3
SROW = 8
NROW = 24
SROWS = 48
MU = 4
SU = 6

VMEM = pl.BlockSpec(memory_space=pltpu.VMEM)


def passed_along(block, axis, distance):
    devices = range(lax.axis_size(axis))
    route = [(i - distance, i) for i in devices if i - distance in devices]
    return lax.ppermute(block, axis, route)


def lane_pairs(bands):
    levels = bands.shape[-1]
    low = jnp.pad(bands[:8], ((0, 0), (0, 0), (0, LANES - levels)))
    high = jnp.pad(bands[8:], ((0, 1), (0, 0), (64, 64 - levels)))
    return low + high


def to_edges(slab, axis):
    size = lax.axis_size(axis)
    t = jnp.transpose(slab, (0, 1, 3, 4, 2))
    first = lane_pairs(t[0].reshape(15, *t.shape[3:]))
    last = lane_pairs(t[1, :, ::-1].reshape(15, *t.shape[3:]))
    zero = jnp.zeros((size - 2, *first.shape), first.dtype)
    sent = jnp.concatenate([first[None], zero, last[None]], axis=0)
    return lax.all_to_all(sent, axis, 0, 0, tiled=True)


def iota8(dim):
    return lax.broadcasted_iota(jnp.int32, (8, LANES), dim)


def axis_ends(axis):
    at = lax.axis_index(axis)
    return at == 0, at == lax.axis_size(axis) - 1


def loop(count, unroll, body, carry):
    assert count % unroll == 0

    def trip(g, carry):
        for i in range(unroll):
            carry = body(g * unroll + i, carry)
        return carry

    return lax.fori_loop(0, count // unroll, trip, carry)


def each(count, unroll, body):
    def step(i, carry):
        body(i)
        return carry

    loop(count, unroll, step, 0)


def side_bands(sng, bs, bt, size_x):
    zero = jnp.zeros((8, LANES), jnp.float32)

    def clear(i):
        for k in range(3):
            bs[k, pl.ds(pl.multiple_of(i * 8, 8), 8), :] = zero

    each(64, 4, clear)
    for s in range(8):
        b = jnp.concatenate([sng[s], jnp.zeros((LANES - size_x, LANES), jnp.float32)], axis=0).T
        for half in range(2):
            kj = s + 8 * half
            if kj < 15:
                bs[kj // 5, pl.ds(kj % 5, 64, stride=8), :] = b[64 * half : 64 * half + 64]
    for k in range(3):
        for g in range(4):
            bt[k, g] = bs[k, g * LANES : (g + 1) * LANES, :].T


def side_weight(ny, width, rows):
    is_south, is_north = axis_ends("gy")
    y = iota8(1).astype(jnp.float32) + (lax.axis_index("gy") * LANES).astype(jnp.float32)
    dist = jnp.where(is_north, (ny - 1.0) - y, y)
    rate = width[rows, :].astype(jnp.float32)
    return jnp.maximum(rate - dist, 0.0) / rate


def side_band(bt, k, z, rows):
    _, is_north = axis_ends("gy")
    base = jnp.where(is_north, 123 + LANES, LANES)
    shift = lax.rem(base - 8 * lax.rem(z, 16), LANES)
    return pltpu.roll(bt[k, z // 16, rows, :], shift, 1)


def rim_kernel(ny, u, v, p, w, coef, width, sng, east, west, bs, bt):
    levels, size_x, _ = u.shape
    is_south, is_north = axis_ends("gy")
    zero = jnp.zeros((8, LANES), jnp.float32)
    for msg, lo in ((east, size_x - HALO), (west, 0)):
        for b in range(3):
            msg[levels, 8 * b : 8 * b + 8, :] = zero
        msg[levels, 0:HALO, :] = coef[lo : lo + HALO, :]

    def plain(z):
        for f, src in enumerate((p, u, v, w)):
            east[z, HALO * f : HALO * f + HALO, :] = src[z, size_x - HALO : size_x, :]
            west[z, HALO * f : HALO * f + HALO, :] = src[z, 0:HALO, :]

    each(levels, 2, plain)

    @pl.when(is_south | is_north)
    def _():
        side_bands(sng, bs, bt, size_x)
        at_e = slice(size_x - 8, size_x)
        at_w = slice(0, 8)
        weight_e = side_weight(ny, width, at_e)
        weight_w = side_weight(ny, width, at_w)

        def sides(z):
            for f, (src, k) in enumerate(((p, 2), (u, 0), (v, 1))):
                val = src[z, at_e, :]
                val = val + weight_e * (side_band(bt, k, z, at_e) - val)
                east[z, HALO * f : HALO * f + HALO, :] = val[8 - HALO :]
                val = src[z, at_w, :]
                val = val + weight_w * (side_band(bt, k, z, at_w) - val)
                west[z, HALO * f : HALO * f + HALO, :] = val[:HALO]

        each(levels, 6, sides)


def blend_kernel(nx, ny, u, v, p, width, weg, sng, ub, vb, pb, cw, ce, bs, bt):
    levels, size_x, _ = u.shape
    blocks = size_x // 8
    groups = weg.shape[0]
    is_south, is_north = axis_ends("gy")
    is_west, is_east = axis_ends("gx")
    zero = jnp.zeros((8, LANES), jnp.float32)
    fields = ((p, pb, 2), (u, ub, 0), (v, vb, 1))

    def take(z):
        for src, dst, _ in fields:
            for b in range(blocks):
                dst[z, 8 * b : 8 * b + 8, :] = src[z, 8 * b : 8 * b + 8, :]

    each(levels, 2, take)

    @pl.when(is_west | is_east)
    def _():
        def clear(i):
            for k in range(3):
                cw[k, pl.ds(pl.multiple_of(i * 8, 8), 8), :] = zero
                ce[k, pl.ds(pl.multiple_of(i * 8, 8), 8), :] = zero

        each(64, 4, clear)
        for s in range(8):
            a = jnp.concatenate([weg[g, s] for g in range(groups)], axis=0).T
            for half in range(2):
                kj = s + 8 * half
                if kj < 15:
                    k, j = kj // 5, kj % 5
                    cw[k, pl.ds(j, 64, stride=8), :] = a[64 * half : 64 * half + 64]
                    ce[k, pl.ds(3 + j, 64, stride=8), :] = a[64 * half : 64 * half + 64]
        x = iota8(0).astype(jnp.float32) + (lax.axis_index("gx") * size_x).astype(jnp.float32)
        rate_w = width[0:8, :].astype(jnp.float32)
        rate_e = width[size_x - 8 : size_x, :].astype(jnp.float32)
        weight_w = jnp.maximum(rate_w - x, 0.0) / rate_w
        weight_e = jnp.maximum(rate_e - ((nx - 1.0) - (x + (size_x - 8.0))), 0.0) / rate_e

        def ends(z):
            rows = pl.ds(pl.multiple_of(z * 8, 8), 8)
            for src, dst, k in fields:
                val = dst[z, 0:8, :]
                dst[z, 0:8, :] = val + weight_w * (cw[k, rows, :] - val)
                val = dst[z, size_x - 8 : size_x, :]
                dst[z, size_x - 8 : size_x, :] = val + weight_e * (ce[k, rows, :] - val)

        each(levels, 3, ends)

    @pl.when(is_south | is_north)
    def _():
        side_bands(sng, bs, bt, size_x)
        for b in range(blocks):
            at = slice(8 * b, 8 * b + 8)
            weight = side_weight(ny, width, at)

            def sides(z):
                for _, dst, k in fields:
                    val = dst[z, at, :]
                    dst[z, at, :] = val + weight * (side_band(bt, k, z, at) - val)

            each(levels, 12 if levels % 12 == 0 else 6, sides)


def strip_kernel(p, u, v, w, coef, from_w, from_e, own, own_r, north, south, halo):
    levels, size_x, _ = u.shape
    blocks = size_x // 8
    zero = jnp.zeros((8, LANES), jnp.float32)
    lane_group = iota8(1) // 16

    for f in range(4):

        def unpack(z):
            halo[f, z, 2:8, :] = from_w[z, HALO * f : HALO * f + HALO, :]
            halo[f, z, 8:14, :] = from_e[z, HALO * f : HALO * f + HALO, :]

        each(levels, 6, unpack)
    halo[4, 0, 2:8, :] = from_w[levels, 0:HALO, :]
    halo[4, 0, 8:14, :] = from_e[levels, 0:HALO, :]

    def turned(parts):
        rows = [zero] + parts + [zero] * (LANES // 8 - 1 - len(parts))
        return jnp.concatenate(rows, axis=0).T

    def group(g, _):
        for f, src in enumerate((p, u, v, w)):
            acc = None
            for zi in range(ZG):
                z = g * ZG + zi
                parts = [halo[f, z, 0:8, :]]
                parts += [src[z, 8 * b : 8 * b + 8, :] for b in range(blocks)]
                parts += [halo[f, z, 8:16, :]]
                parts = [pltpu.roll(part, (8 + 16 * zi) % LANES, 1) for part in parts]
                if acc is None:
                    acc = parts
                else:
                    acc = [jnp.where(lane_group == zi, part, old) for part, old in zip(parts, acc)]
            t = turned(acc)
            for zi in range(ZG):
                z = g * ZG + zi
                both = t[16 * zi : 16 * zi + 16]
                own[f, z] = both
                north[z, HALO * f : HALO * f + HALO, :] = both[2:8]
                south[z, HALO * f : HALO * f + HALO, :] = both[8:14]
        return 0

    lax.fori_loop(0, levels // ZG, group, 0)

    parts = [halo[4, 0, 0:8, :]]
    parts += [coef[8 * b : 8 * b + 8, :] for b in range(blocks)]
    parts += [halo[4, 0, 8:16, :]]
    t = turned([pltpu.roll(part, 8, 1) for part in parts])
    own_r[...] = t[0:16]
    for msg in (north, south):
        for b in range(3):
            msg[levels, 8 * b : 8 * b + 8, :] = zero
    north[levels, 0:HALO, :] = t[2:8]
    south[levels, 0:HALO, :] = t[8:14]


def step_kernel(
    ub, vb, pb, w_in, coef, from_w, from_e, own, own_r, from_s, from_n,
    u_out, v_out, w_out, p_out,
    P_, E_, W_, S_, M_, Q_, R_, sP, sE, sW, sQ, sM, sR, rows, T_,
):
    levels, size_x, _ = ub.shape
    blocks = size_x // 8
    starts = [8 * b for b in range(1, blocks + 3)]
    main = [OFF + 8 * b for b in range(blocks)]
    sstarts = [SROW, SROW + 8, NROW, NROW + 8]
    zero = jnp.zeros((8, LANES), jnp.float32)
    sub = iota8(0)
    lane = iota8(1)
    is_west, is_east = axis_ends("gx")
    is_south, is_north = axis_ends("gy")
    mask_w = (sub == 0) & is_west
    mask_e = (sub == 7) & is_east
    smask_w = (lane == OFF) & is_west
    smask_e = (lane == OFF + size_x - 1) & is_east
    smask_s = (sub == 0) & is_south
    smask_n = (sub == 7) & is_north
    lane0 = lane == 0
    lane127 = lane == LANES - 1
    AB = ACCEL * SPREAD

    def unpack(z):
        for f, src, dst, sdst in ((0, pb, P_, sP), (1, ub, S_, sQ), (2, vb, M_, sM), (3, w_in, W_, sW)):
            scale = 2.0 if f == 3 else 1.0
            lo = HALO * f
            for b in range(blocks):
                dst[z, OFF + 8 * b : OFF + 8 * b + 8, :] = src[z, 8 * b : 8 * b + 8, :] * scale
            dst[z, OFF - HALO : OFF, :] = from_w[z, lo : lo + HALO, :] * scale
            dst[z, OFF + size_x : OFF + size_x + HALO, :] = from_e[z, lo : lo + HALO, :] * scale
            sdst[z, SROW + 8 : SROW + 16, :] = own[f, z, 8:16, :] * scale
            sdst[z, NROW : NROW + 8, :] = own[f, z, 0:8, :] * scale
            sdst[z, SROW + 8 - HALO : SROW + 8, :] = from_s[z, lo : lo + HALO, :] * scale
            sdst[z, NROW + 8 : NROW + 8 + HALO, :] = from_n[z, lo : lo + HALO, :] * scale

    each(levels, 1, unpack)
    R_[OFF : OFF + size_x, :] = coef[...]
    R_[OFF - HALO : OFF, :] = from_w[levels, 0:HALO, :]
    R_[OFF + size_x : OFF + size_x + HALO, :] = from_e[levels, 0:HALO, :]
    sR[SROW + 8 : SROW + 16, :] = own_r[8:16, :]
    sR[NROW : NROW + 8, :] = own_r[0:8, :]
    sR[SROW + 8 - HALO : SROW + 8, :] = from_s[levels, 0:HALO, :]
    sR[NROW + 8 : NROW + 8 + HALO, :] = from_n[levels, 0:HALO, :]

    def strip_init(z):
        for s in sstarts:
            u = sQ[z, s : s + 8, :]
            v = sM[z, s : s + 8, :]
            v_s = sM[z, s - 1 : s + 7, :]
            sE[z, s : s + 8, :] = SPREAD * ((u - pltpu.roll(u, 1, 1)) + (v - v_s))
        rows[SUBSTEPS, pl.ds(2 * z, 1), :] = sM[z, SROW + 7 : SROW + 8, :]

    each(levels, 6, strip_init)

    def factors(coefs, dst, at):
        def body(z, prev):
            new = []
            for s, m in zip(at, prev):
                r = coefs[s : s + 8, :]
                m = 1.0 / (1.0 + 2.0 * r - r * r * m)
                dst[z, s : s + 8, :] = m
                new.append(m)
            return tuple(new)

        lax.fori_loop(0, levels, body, tuple(zero for _ in at))

    factors(sR, sM, sstarts)

    def substep(pp, qq, ww, mm, rr, at, sectioned, size, size_b):
        def down(z, qs, ds, last=False):
            new = []
            qn = None if last else [qq[z + 1, s : s + 8, :] for s in at]
            for i, s in enumerate(at):
                rhs = ww[z, s : s + 8, :] + (qs[i] if last else qs[i] - qn[i])
                if ds is not None:
                    rhs = rhs + rr[s : s + 8, :] * ds[i]
                d = mm[z, s : s + 8, :] * rhs
                ww[z, s : s + 8, :] = d
                new.append(d)
            return qn, tuple(new)

        groups = levels // size
        for i in range(size):
            sectioned(i)
        for i in range(size):
            sectioned(size + i)
        qs = [qq[0, s : s + 8, :] for s in at]
        ds = None
        for i in range(size - 1):
            qs, ds = down(i, qs, ds)

        def fwd(g, ds):
            for i in range(size):
                sectioned((g + 1) * size + i)
            qs = [qq[g * size - 1, s : s + 8, :] for s in at]
            for i in range(size):
                qs, ds = down(g * size - 1 + i, qs, ds)
            return ds

        ds = lax.fori_loop(1, groups - 1, fwd, ds)
        first = (groups - 1) * size - 1
        qs = [qq[first, s : s + 8, :] for s in at]
        for i in range(size):
            qs, ds = down(first + i, qs, ds)
        _, ws = down(levels - 1, qs, ds, last=True)

        def up(z, ws):
            new = []
            for j, s in enumerate(at):
                w = ww[z, s : s + 8, :] + mm[z, s : s + 8, :] * (rr[s : s + 8, :] * ws[j])
                ww[z, s : s + 8, :] = w
                pp[z + 1, s : s + 8, :] = qq[z + 1, s : s + 8, :] - 0.25 * (ws[j] - w)
                new.append(w)
            return tuple(new)

        for i in range(size_b - 1):
            ws = up(levels - 2 - i, ws)

        def bwd(g, ws):
            for i in range(size_b):
                ws = up(levels - 1 - size_b - g * size_b - i, ws)
            return ws

        ws = lax.fori_loop(0, levels // size_b - 1, bwd, ws)
        for j, s in enumerate(at):
            pp[0, s : s + 8, :] = qq[0, s : s + 8, :] - 0.25 * ws[j]

    def strip_step(k, _):
        def sectioned(z):
            for s in sstarts:
                p = sP[z, s : s + 8, :]
                p_s = sP[z, s - 1 : s + 7, :]
                p_n = sP[z, s + 1 : s + 9, :]
                p_w = jnp.where(smask_w, p, pltpu.roll(p, 1, 1))
                p_e = jnp.where(smask_e, 0.0, pltpu.roll(p, LANES - 1, 1))
                if s == SROW + 8:
                    p_s = jnp.where(smask_s, p, p_s)
                if s == NROW:
                    p_n = jnp.where(smask_n, 0.0, p_n)
                e = sE[z, s : s + 8, :] - AB * (((p_w + p_e) + (p_s + p_n)) - 4.0 * p)
                sE[z, s : s + 8, :] = e
                sQ[z, s : s + 8, :] = p - e
            edge_s = jnp.where(is_south, sP[z, SROW + 8 : SROW + 9, :], sP[z, SROW + 7 : SROW + 8, :])
            edge_n = jnp.where(is_north, 0.0, sP[z, NROW + 8 : NROW + 9, :])
            rows[k, pl.ds(2 * z, 1), :] = edge_s
            rows[k, pl.ds(lax.rem(2 * z + LANES - 1, LANES), 1), :] = edge_n

        substep(sP, sQ, sW, sM, sR, sstarts, sectioned, SU, 6)
        return 0

    lax.fori_loop(0, SUBSTEPS, strip_step, 0)

    for k in range(SUBSTEPS + 1):
        T_[k] = rows[k].T

    def edges(k, z, s):
        return pltpu.roll(T_[k, s : s + 8, :], lax.rem(2 * LANES - 2 * z, LANES), 1)

    def main_init(z):
        for s in starts:
            u = S_[z, s : s + 8, :]
            u_w = S_[z, s - 1 : s + 7, :]
            v = M_[z, s : s + 8, :]
            v_s = jnp.where(lane0, edges(SUBSTEPS, z, s), pltpu.roll(v, 1, 1))
            E_[z, s : s + 8, :] = SPREAD * ((u - u_w) + (v - v_s))

    each(levels, 3, main_init)

    def clear(z):
        for s in starts[1:]:
            S_[z, s : s + 8, :] = zero

    each(levels, 3, clear)
    factors(R_, M_, starts)

    def main_step(k, _):
        def sectioned(z):
            for s in starts:
                p = P_[z, s : s + 8, :]
                p_w = P_[z, s - 1 : s + 7, :]
                p_e = P_[z, s + 1 : s + 9, :]
                if s == main[0]:
                    p_w = jnp.where(mask_w, p, p_w)
                if s == main[-1]:
                    p_e = jnp.where(mask_e, 0.0, p_e)
                edge = edges(k, z, s)
                p_s = jnp.where(lane0, edge, pltpu.roll(p, 1, 1))
                p_n = jnp.where(lane127, edge, pltpu.roll(p, LANES - 1, 1))
                e = E_[z, s : s + 8, :] - AB * (((p_w + p_e) + (p_s + p_n)) - 4.0 * p)
                E_[z, s : s + 8, :] = e
                if s != starts[0]:
                    S_[z, s : s + 8, :] = S_[z, s : s + 8, :] + p
                Q_[z, s : s + 8, :] = p - e

        substep(P_, Q_, W_, M_, R_, starts, sectioned, MU, 3)
        return 0

    lax.fori_loop(0, SUBSTEPS, main_step, 0)

    total = T_[0]
    for k in range(1, SUBSTEPS):
        total = total + T_[k]
    T_[0] = total

    def finish(z):
        for b, s in enumerate(main):
            at = slice(8 * b, 8 * b + 8)
            total = S_[z, s : s + 8, :]
            east = S_[z, s + 1 : s + 9, :]
            if s == main[-1]:
                east = jnp.where(mask_e, 0.0, east)
            north = jnp.where(lane127, edges(0, z, s), pltpu.roll(total, LANES - 1, 1))
            u_out[z, at, :] = ub[z, at, :] - ACCEL * (east - total)
            v_out[z, at, :] = vb[z, at, :] - ACCEL * (north - total)
            w_out[z, at, :] = 0.5 * W_[z, s : s + 8, :]
            p_out[z, at, :] = P_[z, s : s + 8, :]

    each(levels, 3, finish)


def per_device(u_wind, v_wind, w_wind, pressure, vert_coef, we_slab, sn_slab, relax_width):
    levels, size_x, size_y = pressure.shape
    nx = float(size_x * lax.axis_size("gx"))
    ny = float(size_y * lax.axis_size("gy"))
    weg = to_edges(we_slab, "gx")
    sng = to_edges(sn_slab, "gy")
    sng = jnp.transpose(sng, (1, 0, 2, 3)).reshape(8, size_x, LANES)
    f32 = jnp.float32
    block = jax.ShapeDtypeStruct(pressure.shape, f32)
    message = jax.ShapeDtypeStruct((levels + 1, 4 * HALO, LANES), f32)
    ext = size_x + 2 * OFF

    bands = pltpu.VMEM((3, 512, LANES), f32)
    turned = pltpu.VMEM((3, 4, LANES, LANES), f32)
    east, west = pl.pallas_call(
        lambda *refs: rim_kernel(ny, *refs),
        out_shape=(message, message),
        in_specs=[VMEM] * 7,
        out_specs=[VMEM] * 2,
        scratch_shapes=[bands, turned],
        compiler_params=pltpu.CompilerParams(vmem_limit_bytes=24 << 20),
        name="rims",
    )(u_wind, v_wind, pressure, w_wind, vert_coef, relax_width, sng)
    ub, vb, pb = pl.pallas_call(
        lambda *refs: blend_kernel(nx, ny, *refs),
        out_shape=(block, block, block),
        in_specs=[VMEM] * 6,
        out_specs=[VMEM] * 3,
        scratch_shapes=[bands, bands, bands, turned],
        compiler_params=pltpu.CompilerParams(vmem_limit_bytes=24 << 20),
        name="blend",
    )(u_wind, v_wind, pressure, relax_width, weg, sng)
    from_w = passed_along(east, "gx", 1)
    from_e = passed_along(west, "gx", -1)

    own, own_r, north, south = pl.pallas_call(
        strip_kernel,
        out_shape=(
            jax.ShapeDtypeStruct((4, levels, 16, LANES), f32),
            jax.ShapeDtypeStruct((16, LANES), f32),
            message,
            message,
        ),
        in_specs=[VMEM] * 7,
        out_specs=[VMEM] * 4,
        scratch_shapes=[pltpu.VMEM((5, levels, 16, LANES), f32)],
        compiler_params=pltpu.CompilerParams(vmem_limit_bytes=24 << 20),
        name="strips",
    )(pb, ub, vb, w_wind, vert_coef, from_w, from_e)
    from_s = passed_along(north, "gy", 1)
    from_n = passed_along(south, "gy", -1)

    big = pltpu.VMEM((levels, ext, LANES), f32)
    strip = pltpu.VMEM((levels, SROWS, LANES), f32)
    return pl.pallas_call(
        step_kernel,
        out_shape=(block, block, block, block),
        in_specs=[VMEM] * 11,
        out_specs=[VMEM] * 4,
        scratch_shapes=[big] * 6
        + [pltpu.VMEM((ext, LANES), f32)]
        + [strip] * 5
        + [
            pltpu.VMEM((SROWS, LANES), f32),
            pltpu.VMEM((SUBSTEPS + 1, LANES, LANES), f32),
            pltpu.VMEM((SUBSTEPS + 1, LANES, LANES), f32),
        ],
        compiler_params=pltpu.CompilerParams(vmem_limit_bytes=40 << 20),
        name="substeps",
    )(ub, vb, pb, w_wind, vert_coef, from_w, from_e, own, own_r, from_s, from_n)


def solution(mesh):
    placed = (
        P(None, "gx", "gy"),
        P(None, "gx", "gy"),
        P(None, "gx", "gy"),
        P(None, "gx", "gy"),
        P("gx", "gy"),
        P(None, None, None, None, ("gy", "gx")),
        P(None, None, None, None, ("gx", "gy")),
        P("gx", "gy"),
    )
    return jax.shard_map(
        per_device,
        mesh=mesh,
        in_specs=placed,
        out_specs=(P(None, "gx", "gy"),) * 4,
        check_vma=False,
    )
```

```python
import jax
import jax.numpy as jnp
from jax import lax
from jax.experimental import pallas as pl
from jax.experimental.pallas import tpu as pltpu
from jax.sharding import PartitionSpec as P


SUBSTEPS = 6
HALO = 6
OFF = 16
ZG = 6
SB = 5
ZS = 12
LANES = 128
ACCEL = 0.3
SPREAD = 0.3
SROW = 8
NROW = 24
SROWS = 48
MU = 10
SU = 12

VMEM = pl.BlockSpec(memory_space=pltpu.VMEM)
HBM = pl.BlockSpec(memory_space=pltpu.HBM)


def passed_along(block, axis, distance):
    devices = range(lax.axis_size(axis))
    route = [(i - distance, i) for i in devices if i - distance in devices]
    return lax.ppermute(block, axis, route)


def lane_pairs(bands):
    levels = bands.shape[-1]
    low = jnp.pad(bands[:8], ((0, 0), (0, 0), (0, LANES - levels)))
    high = jnp.pad(bands[8:], ((0, 1), (0, 0), (64, 64 - levels)))
    return low + high


def to_edges(slab, axis):
    size = lax.axis_size(axis)
    t = jnp.transpose(slab, (0, 1, 3, 4, 2))
    first = lane_pairs(t[0].reshape(15, *t.shape[3:]))
    last = lane_pairs(t[1, :, ::-1].reshape(15, *t.shape[3:]))
    zero = jnp.zeros((size - 2, *first.shape), first.dtype)
    sent = jnp.concatenate([first[None], zero, last[None]], axis=0)
    return lax.all_to_all(sent, axis, 0, 0, tiled=True)


def iota8(dim):
    return lax.broadcasted_iota(jnp.int32, (8, LANES), dim)


def axis_ends(axis):
    at = lax.axis_index(axis)
    return at == 0, at == lax.axis_size(axis) - 1


def loop(count, unroll, body, carry):
    assert count % unroll == 0

    def trip(g, carry):
        for i in range(unroll):
            carry = body(g * unroll + i, carry)
        return carry

    return lax.fori_loop(0, count // unroll, trip, carry)


def each(count, unroll, body):
    def step(i, carry):
        body(i)
        return carry

    loop(count, unroll, step, 0)


def side_bands(sn_w, sng, sn_e, bs, bt):
    zero = jnp.zeros((8, LANES), jnp.float32)
    spare = jnp.zeros((LANES - 16 - sng.shape[1], LANES), jnp.float32)

    def clear(i):
        for k in range(3):
            bs[k, pl.ds(pl.multiple_of(i * 8, 8), 8), :] = zero

    each(64, 4, clear)
    for s in range(8):
        b = jnp.concatenate([sn_w[s], sng[s], sn_e[s], spare], axis=0).T
        for half in range(2):
            kj = s + 8 * half
            if kj < 15:
                bs[kj // 5, pl.ds(kj % 5, 64, stride=8), :] = b[64 * half : 64 * half + 64]
    for k in range(3):
        for g in range(4):
            bt[k, g] = bs[k, g * LANES : (g + 1) * LANES, :].T


def end_bands(weg, cw, ce):
    groups = weg.shape[0]
    zero = jnp.zeros((8, LANES), jnp.float32)

    def clear(i):
        for k in range(3):
            cw[k, pl.ds(pl.multiple_of(i * 8, 8), 8), :] = zero
            ce[k, pl.ds(pl.multiple_of(i * 8, 8), 8), :] = zero

    each(64, 4, clear)
    for s in range(8):
        a = jnp.concatenate([weg[g, s] for g in range(groups)], axis=0).T
        for half in range(2):
            kj = s + 8 * half
            if kj < 15:
                k, j = kj // 5, kj % 5
                cw[k, pl.ds(j, 64, stride=8), :] = a[64 * half : 64 * half + 64]
                ce[k, pl.ds(3 + j, 64, stride=8), :] = a[64 * half : 64 * half + 64]


def rim_kernel(p, u, v, w, coef, width, east, west, held, sems):
    levels, size_x, _ = u.shape
    zero = jnp.zeros((8, LANES), jnp.float32)
    copies = []
    for f, src in enumerate((p, u, v, w)):
        for side, lo in enumerate((size_x - 8, 0)):
            copies.append(pltpu.make_async_copy(src.at[:, lo : lo + 8, :], held.at[side, f], sems.at[side, f]))
    for copy in copies:
        copy.start()
    for msg, lo in ((east, size_x - HALO), (west, 0)):
        for b in range(3):
            msg[levels, 8 * b : 8 * b + 8, :] = zero
        msg[levels, 0:HALO, :] = coef[lo : lo + HALO, :]
        msg[levels, HALO : 2 * HALO, :] = width[lo : lo + HALO, :].astype(jnp.float32)
    for copy in copies:
        copy.wait()

    def pack(z):
        for f in range(4):
            east[z, HALO * f : HALO * f + HALO, :] = held[0, f, z, 8 - HALO : 8, :]
            west[z, HALO * f : HALO * f + HALO, :] = held[1, f, z, 0:HALO, :]

    each(levels, 4, pack)


def strip_kernel(
    nx, ny, p, u, v, w, coef, width, weg, sn_w, sng, sn_e, from_w, from_e,
    px, ux, vx, wx, halo_r, own, own_r, north, south,
    cw, ce, bs, bt, rate_, sems,
):
    levels, size_x, _ = u.shape
    blocks = size_x // 8
    starts = [OFF - 8 + 8 * b for b in range(blocks + 2)]
    ends_at = (OFF, OFF + size_x - 8)
    zero = jnp.zeros((8, LANES), jnp.float32)
    is_west, is_east = axis_ends("gx")
    is_south, is_north = axis_ends("gy")
    fields = ((p, px, 2), (u, ux, 0), (v, vx, 1), (w, wx, None))
    copies = [
        pltpu.make_async_copy(src, dst.at[:, OFF : OFF + size_x, :], sems.at[f])
        for f, (src, dst, _) in enumerate(fields)
    ]
    for copy in copies:
        copy.start()

    for f, (_, dst, _) in enumerate(fields):

        def unpack(z):
            dst[z, OFF - HALO : OFF, :] = from_w[z, HALO * f : HALO * f + HALO, :]
            dst[z, OFF + size_x : OFF + size_x + HALO, :] = from_e[z, HALO * f : HALO * f + HALO, :]

        each(levels, 6, unpack)
    halo_r[2:8, :] = from_w[levels, 0:HALO, :]
    halo_r[8:14, :] = from_e[levels, 0:HALO, :]

    @pl.when(is_west | is_east)
    def _():
        end_bands(weg, cw, ce)

    @pl.when(is_south | is_north)
    def _():
        side_bands(sn_w, sng, sn_e, bs, bt)
        rate_[2:8, :] = from_w[levels, HALO : 2 * HALO, :]
        rate_[8 : 8 + size_x, :] = width[...].astype(jnp.float32)
        rate_[8 + size_x : 14 + size_x, :] = from_e[levels, HALO : 2 * HALO, :]

    def ends(dst, k):
        x = iota8(0).astype(jnp.float32) + (lax.axis_index("gx") * size_x).astype(jnp.float32)
        rate_w = width[0:8, :].astype(jnp.float32)
        rate_e = width[size_x - 8 : size_x, :].astype(jnp.float32)
        weight_w = jnp.maximum(rate_w - x, 0.0) / rate_w
        weight_e = jnp.maximum(rate_e - ((nx - 1.0) - (x + (size_x - 8.0))), 0.0) / rate_e

        def body(z):
            rows = pl.ds(pl.multiple_of(z * 8, 8), 8)
            for at, weight, band in zip(ends_at, (weight_w, weight_e), (cw, ce)):
                val = dst[z, at : at + 8, :]
                dst[z, at : at + 8, :] = val + weight * (band[k, rows, :] - val)

        each(levels, 6, body)

    def sides(dst, k):
        y = iota8(1).astype(jnp.float32) + (lax.axis_index("gy") * LANES).astype(jnp.float32)
        dist = jnp.where(is_north, (ny - 1.0) - y, y)
        base = jnp.where(is_north, 123 + LANES, LANES)
        for first in range(0, blocks + 2, SB):
            some = range(first, min(first + SB, blocks + 2))
            weights = []
            for b in some:
                rate = jnp.maximum(rate_[8 * b : 8 * b + 8, :], 1.0)
                weights.append(jnp.maximum(rate - dist, 0.0) / rate)

            def trip(g, _):
                new = []
                for i in range(ZS):
                    z = g * ZS + i
                    shift = lax.rem(base - 8 * lax.rem(z, 16), LANES)
                    for b, weight in zip(some, weights):
                        band = pltpu.roll(bt[k, z // 16, 8 * b : 8 * b + 8, :], shift, 1)
                        val = dst[z, starts[b] : starts[b] + 8, :]
                        new.append(val + weight * (band - val))
                for i in range(ZS):
                    for j, b in enumerate(some):
                        dst[g * ZS + i, starts[b] : starts[b] + 8, :] = new[i * len(some) + j]
                return 0

            lax.fori_loop(0, levels // ZS, trip, 0)

    lane_group = iota8(1) // 16

    def turned(parts):
        rows = [zero] + parts + [zero] * (LANES // 8 - 1 - len(parts))
        return jnp.concatenate(rows, axis=0).T

    for f, (_, dst, k) in enumerate(fields):
        copies[f].wait()
        if k is not None:

            @pl.when(is_west | is_east)
            def _():
                ends(dst, k)

            @pl.when(is_south | is_north)
            def _():
                sides(dst, k)

        def group(g, _):
            acc = None
            for zi in range(ZG):
                z = g * ZG + zi
                parts = [dst[z, s : s + 8, :] for s in starts]
                if k is None:
                    parts = [2.0 * part for part in parts]
                    for s, part in zip(starts, parts):
                        dst[z, s : s + 8, :] = part
                parts = [pltpu.roll(part, (8 + 16 * zi) % LANES, 1) for part in parts]
                if acc is None:
                    acc = parts
                else:
                    acc = [jnp.where(lane_group == zi, part, old) for part, old in zip(parts, acc)]
            t = turned(acc)
            for zi in range(ZG):
                z = g * ZG + zi
                both = t[16 * zi : 16 * zi + 16]
                own[f, z] = both
                north[z, HALO * f : HALO * f + HALO, :] = both[2:8]
                south[z, HALO * f : HALO * f + HALO, :] = both[8:14]
            return 0

        lax.fori_loop(0, levels // ZG, group, 0, unroll=2)

    parts = [halo_r[0:8, :]]
    parts += [coef[8 * b : 8 * b + 8, :] for b in range(blocks)]
    parts += [halo_r[8:16, :]]
    t = turned([pltpu.roll(part, 8, 1) for part in parts])
    own_r[...] = t[0:16]
    for msg in (north, south):
        for b in range(3):
            msg[levels, 8 * b : 8 * b + 8, :] = zero
    north[levels, 0:HALO, :] = t[2:8]
    south[levels, 0:HALO, :] = t[8:14]


def step_kernel(
    px, ux, vx, wx, coef, halo_r, own, own_r, from_s, from_n,
    u_out, v_out, w_out, p_out,
    P_, E_, W_, S_, M_, Q_, R_, sP, sE, sW, sQ, sM, sR, rows, T_, sems,
):
    levels, size_x, _ = u_out.shape
    blocks = size_x // 8
    starts = [8 * b for b in range(1, blocks + 3)]
    main = [OFF + 8 * b for b in range(blocks)]
    sstarts = [SROW, SROW + 8, NROW, NROW + 8]
    zero = jnp.zeros((8, LANES), jnp.float32)
    sub = iota8(0)
    lane = iota8(1)
    is_west, is_east = axis_ends("gx")
    is_south, is_north = axis_ends("gy")
    mask_w = (sub == 0) & is_west
    mask_e = (sub == 7) & is_east
    smask_w = (lane == OFF) & is_west
    smask_e = (lane == OFF + size_x - 1) & is_east
    smask_s = (sub == 0) & is_south
    smask_n = (sub == 7) & is_north
    lane0 = lane == 0
    lane127 = lane == LANES - 1
    AB = ACCEL * SPREAD

    def unpack(z):
        for f, dst in enumerate((sP, sQ, sM, sW)):
            lo = HALO * f
            dst[z, SROW + 8 : SROW + 16, :] = own[f, z, 8:16, :]
            dst[z, NROW : NROW + 8, :] = own[f, z, 0:8, :]
            dst[z, SROW + 8 - HALO : SROW + 8, :] = from_s[z, lo : lo + HALO, :]
            dst[z, NROW + 8 : NROW + 8 + HALO, :] = from_n[z, lo : lo + HALO, :]

    each(levels, 2, unpack)
    R_[OFF : OFF + size_x, :] = coef[...]
    R_[OFF - 8 : OFF, :] = halo_r[0:8, :]
    R_[OFF + size_x : OFF + size_x + 8, :] = halo_r[8:16, :]
    sR[SROW + 8 : SROW + 16, :] = own_r[8:16, :]
    sR[NROW : NROW + 8, :] = own_r[0:8, :]
    sR[SROW + 8 - HALO : SROW + 8, :] = from_s[levels, 0:HALO, :]
    sR[NROW + 8 : NROW + 8 + HALO, :] = from_n[levels, 0:HALO, :]

    def strip_init(z):
        for s in sstarts:
            u = sQ[z, s : s + 8, :]
            v = sM[z, s : s + 8, :]
            v_s = sM[z, s - 1 : s + 7, :]
            sE[z, s : s + 8, :] = SPREAD * ((u - pltpu.roll(u, 1, 1)) + (v - v_s))
        rows[SUBSTEPS, pl.ds(2 * z, 1), :] = sM[z, SROW + 7 : SROW + 8, :]

    each(levels, 6, strip_init)

    def factors(coefs, dst, at):
        def body(z, prev):
            new = []
            for s, m in zip(at, prev):
                r = coefs[s : s + 8, :]
                m = 1.0 / (1.0 + 2.0 * r - r * r * m)
                dst[z, s : s + 8, :] = m
                new.append(m)
            return tuple(new)

        lax.fori_loop(0, levels, body, tuple(zero for _ in at))

    factors(sR, sM, sstarts)

    def descend(qq, ww, mm, rr, at, sectioned, size):
        def down(z, qs, ds, last=False):
            new = []
            qn = None if last else [qq[z + 1, s : s + 8, :] for s in at]
            for i, s in enumerate(at):
                rhs = ww[z, s : s + 8, :] + (qs[i] if last else qs[i] - qn[i])
                if ds is not None:
                    rhs = rhs + rr[s : s + 8, :] * ds[i]
                d = mm[z, s : s + 8, :] * rhs
                ww[z, s : s + 8, :] = d
                new.append(d)
            return qn, tuple(new)

        groups = levels // size
        for i in range(2 * size):
            sectioned(i)
        qs = [qq[0, s : s + 8, :] for s in at]
        ds = None
        for i in range(size - 1):
            qs, ds = down(i, qs, ds)

        def fwd(g, ds):
            qs = [qq[g * size - 1, s : s + 8, :] for s in at]
            for i in range(size):
                qs, ds = down(g * size - 1 + i, qs, ds)
            for i in range(size):
                sectioned((g + 1) * size + i)
            return ds

        ds = lax.fori_loop(1, groups - 1, fwd, ds)
        first = (groups - 1) * size - 1
        qs = [qq[first, s : s + 8, :] for s in at]
        for i in range(size):
            qs, ds = down(first + i, qs, ds)
        return down(levels - 1, qs, ds, last=True)[1]

    def ascend(pp, qq, ww, mm, rr, at, ws, size, scale=1.0, done=None):
        def up(z, ws):
            new = []
            for j, s in enumerate(at):
                w = ww[z, s : s + 8, :] + mm[z, s : s + 8, :] * (rr[s : s + 8, :] * ws[j])
                ww[z, s : s + 8, :] = w if scale == 1.0 else scale * w
                pp[z + 1, s : s + 8, :] = qq[z + 1, s : s + 8, :] - 0.25 * (ws[j] - w)
                new.append(w)
            return tuple(new)

        chunk = levels // 4 if done else levels
        if scale != 1.0:
            for j, s in enumerate(at):
                ww[levels - 1, s : s + 8, :] = scale * ws[j]
        for hi in range(levels, 0, -chunk):
            top = hi - 1
            left = chunk
            if hi == levels:
                for i in range(size - 1):
                    ws = up(levels - 2 - i, ws)
                top = levels - 1 - size
                left = chunk - size

            def bwd(g, ws):
                for i in range(size):
                    ws = up(top - g * size - i, ws)
                return ws

            ws = lax.fori_loop(0, left // size, bwd, ws)
            if hi == chunk:
                for j, s in enumerate(at):
                    pp[0, s : s + 8, :] = qq[0, s : s + 8, :] - 0.25 * ws[j]
            if done:
                done(hi - chunk, hi)

    def strip_step(k, _):
        def sectioned(z):
            for s in sstarts:
                p = sP[z, s : s + 8, :]
                p_s = sP[z, s - 1 : s + 7, :]
                p_n = sP[z, s + 1 : s + 9, :]
                p_w = jnp.where(smask_w, p, pltpu.roll(p, 1, 1))
                p_e = jnp.where(smask_e, 0.0, pltpu.roll(p, LANES - 1, 1))
                if s == SROW + 8:
                    p_s = jnp.where(smask_s, p, p_s)
                if s == NROW:
                    p_n = jnp.where(smask_n, 0.0, p_n)
                e = sE[z, s : s + 8, :] - AB * (((p_w + p_e) + (p_s + p_n)) - 4.0 * p)
                sE[z, s : s + 8, :] = e
                sQ[z, s : s + 8, :] = p - e
            edge_s = jnp.where(is_south, sP[z, SROW + 8 : SROW + 9, :], sP[z, SROW + 7 : SROW + 8, :])
            edge_n = jnp.where(is_north, 0.0, sP[z, NROW + 8 : NROW + 9, :])
            rows[k, pl.ds(2 * z, 1), :] = edge_s
            rows[k, pl.ds(lax.rem(2 * z + LANES - 1, LANES), 1), :] = edge_n

        ws = descend(sQ, sW, sM, sR, sstarts, sectioned, SU)
        ascend(sP, sQ, sW, sM, sR, sstarts, ws, 6)
        return 0

    lax.fori_loop(0, SUBSTEPS, strip_step, 0)

    for k in range(SUBSTEPS + 1):
        T_[k] = rows[k].T

    def edges(k, z, s):
        return pltpu.roll(T_[k, s : s + 8, :], lax.rem(2 * LANES - 2 * z, LANES), 1)

    def main_init(z):
        for s in starts:
            u = ux[z, s : s + 8, :]
            u_w = ux[z, s - 1 : s + 7, :]
            v = vx[z, s : s + 8, :]
            v_s = jnp.where(lane0, edges(SUBSTEPS, z, s), pltpu.roll(v, 1, 1))
            E_[z, s : s + 8, :] = SPREAD * ((u - u_w) + (v - v_s))
            P_[z, s : s + 8, :] = px[z, s : s + 8, :]
            W_[z, s : s + 8, :] = wx[z, s : s + 8, :]
            if s != starts[0]:
                S_[z, s : s + 8, :] = zero

    each(levels, 6, main_init)
    factors(R_, M_, starts)

    def main_down(k):
        def sectioned(z):
            for s in starts:
                p = P_[z, s : s + 8, :]
                p_w = P_[z, s - 1 : s + 7, :]
                p_e = P_[z, s + 1 : s + 9, :]
                if s == main[0]:
                    p_w = jnp.where(mask_w, p, p_w)
                if s == main[-1]:
                    p_e = jnp.where(mask_e, 0.0, p_e)
                edge = edges(k, z, s)
                p_s = jnp.where(lane0, edge, pltpu.roll(p, 1, 1))
                p_n = jnp.where(lane127, edge, pltpu.roll(p, LANES - 1, 1))
                e = E_[z, s : s + 8, :] - AB * (((p_w + p_e) + (p_s + p_n)) - 4.0 * p)
                E_[z, s : s + 8, :] = e
                if s != starts[0]:
                    S_[z, s : s + 8, :] = S_[z, s : s + 8, :] + p
                Q_[z, s : s + 8, :] = p - e

        return descend(Q_, W_, M_, R_, starts, sectioned, MU)

    def main_step(k, _):
        ws = main_down(k)
        ascend(P_, Q_, W_, M_, R_, starts, ws, 3)
        return 0

    lax.fori_loop(0, SUBSTEPS - 1, main_step, 0)
    ws = main_down(SUBSTEPS - 1)

    total = T_[0]
    for k in range(1, SUBSTEPS):
        total = total + T_[k]
    T_[0] = total

    chunk = levels // 4
    copies = []

    def send(src, dst, lo, hi):
        at = slice(OFF, OFF + size_x)
        copy = pltpu.make_async_copy(src.at[lo:hi, at, :], dst.at[lo:hi], sems.at[len(copies)])
        copy.start()
        copies.append(copy)

    def finish(z):
        for s in main:
            total = S_[z, s : s + 8, :]
            east = S_[z, s + 1 : s + 9, :]
            if s == main[-1]:
                east = jnp.where(mask_e, 0.0, east)
            north = jnp.where(lane127, edges(0, z, s), pltpu.roll(total, LANES - 1, 1))
            E_[z, s : s + 8, :] = ux[z, s : s + 8, :] - ACCEL * (east - total)
            S_[z, s : s + 8, :] = vx[z, s : s + 8, :] - ACCEL * (north - total)

    for c in range(4):
        each(chunk, chunk if chunk < 5 else 5, lambda i: finish(c * chunk + i))
        send(E_, u_out, c * chunk, (c + 1) * chunk)
        send(S_, v_out, c * chunk, (c + 1) * chunk)

    def done(lo, hi):
        send(W_, w_out, lo, hi)
        send(P_, p_out, lo + 1 if lo else 0, min(hi + 1, levels))

    ascend(P_, Q_, W_, M_, R_, main, ws[1 : 1 + blocks], chunk if chunk < 5 else 5, 0.5, done)
    for copy in copies:
        copy.wait()


def whole(u_wind, v_wind, w_wind, pressure, vert_coef, we_slab, sn_slab, relax_width):
    levels, size_x, size_y = pressure.shape
    stay = [pltpu.with_memory_space_constraint(x, pltpu.HBM) for x in (pressure, u_wind, v_wind, w_wind)]
    nx = float(size_x * lax.axis_size("gx"))
    ny = float(size_y * lax.axis_size("gy"))
    f32 = jnp.float32
    block = jax.ShapeDtypeStruct(pressure.shape, f32)
    message = jax.ShapeDtypeStruct((levels + 1, 4 * HALO, LANES), f32)
    ext = size_x + 2 * OFF
    extended = jax.ShapeDtypeStruct((levels, ext, LANES), f32)

    east, west = pl.pallas_call(
        rim_kernel,
        out_shape=(message, message),
        in_specs=[HBM] * 4 + [VMEM] * 2,
        out_specs=[VMEM] * 2,
        scratch_shapes=[
            pltpu.VMEM((2, 4, levels, 8, LANES), f32),
            pltpu.SemaphoreType.DMA((2, 4)),
        ],
        compiler_params=pltpu.CompilerParams(vmem_limit_bytes=24 << 20),
        name="rims",
    )(*stay, vert_coef, relax_width)
    from_w = passed_along(east, "gx", 1)
    from_e = passed_along(west, "gx", -1)

    sng = to_edges(sn_slab, "gy")
    sng = jnp.transpose(sng, (1, 0, 2, 3)).reshape(8, size_x, LANES)
    sn_w = passed_along(sng[:, size_x - 8 :], "gx", 1)
    sn_e = passed_along(sng[:, :8], "gx", -1)
    weg = to_edges(we_slab, "gx")

    bands = pltpu.VMEM((3, 512, LANES), f32)
    px, ux, vx, wx, halo_r, own, own_r, north, south = pl.pallas_call(
        lambda *refs: strip_kernel(nx, ny, *refs),
        out_shape=(
            extended,
            extended,
            extended,
            extended,
            jax.ShapeDtypeStruct((16, LANES), f32),
            jax.ShapeDtypeStruct((4, levels, 16, LANES), f32),
            jax.ShapeDtypeStruct((16, LANES), f32),
            message,
            message,
        ),
        in_specs=[HBM] * 4 + [VMEM] * 8,
        out_specs=[VMEM] * 9,
        scratch_shapes=[
            bands,
            bands,
            bands,
            pltpu.VMEM((3, 4, LANES, LANES), f32),
            pltpu.VMEM((size_x + 16, LANES), f32),
            pltpu.SemaphoreType.DMA((4,)),
        ],
        compiler_params=pltpu.CompilerParams(vmem_limit_bytes=24 << 20),
        name="strips",
    )(*stay, vert_coef, relax_width, weg, sn_w, sng, sn_e, from_w, from_e)
    from_s = passed_along(north, "gy", 1)
    from_n = passed_along(south, "gy", -1)

    big = pltpu.VMEM((levels, ext, LANES), f32)
    strip = pltpu.VMEM((levels, SROWS, LANES), f32)
    return pl.pallas_call(
        step_kernel,
        out_shape=(block, block, block, block),
        in_specs=[VMEM] * 10,
        out_specs=[HBM] * 4,
        scratch_shapes=[big] * 6
        + [pltpu.VMEM((ext, LANES), f32)]
        + [strip] * 5
        + [
            pltpu.VMEM((SROWS, LANES), f32),
            pltpu.VMEM((SUBSTEPS + 1, LANES, LANES), f32),
            pltpu.VMEM((SUBSTEPS + 1, LANES, LANES), f32),
            pltpu.SemaphoreType.DMA((16,)),
        ],
        compiler_params=pltpu.CompilerParams(vmem_limit_bytes=32 << 20),
        name="substeps",
    )(px, ux, vx, wx, vert_coef, halo_r, own, own_r, from_s, from_n)


def solution(mesh):
    placed = (
        P(None, "gx", "gy"),
        P(None, "gx", "gy"),
        P(None, "gx", "gy"),
        P(None, "gx", "gy"),
        P("gx", "gy"),
        P(None, None, None, None, ("gy", "gx")),
        P(None, None, None, None, ("gx", "gy")),
        P("gx", "gy"),
    )
    return jax.shard_map(
        whole,
        mesh=mesh,
        in_specs=placed,
        out_specs=(P(None, "gx", "gy"),) * 4,
        check_vma=False,
    )
```

```python
import jax
import jax.numpy as jnp
from jax import lax
from jax.experimental import pallas as pl
from jax.experimental.pallas import tpu as pltpu
from jax.sharding import PartitionSpec as P


SUBSTEPS = 6
HALO = 6
OFF = 16
ZG = 6
SB = 5
ZS = 12
LANES = 128
ACCEL = 0.3
SPREAD = 0.3
SROW = 8
NROW = 24
SROWS = 48
MU = 10
FU = 6
MB = 10
SU = 12

VMEM = pl.BlockSpec(memory_space=pltpu.VMEM)
HBM = pl.BlockSpec(memory_space=pltpu.HBM)


def passed_along(block, axis, distance):
    devices = range(lax.axis_size(axis))
    route = [(i - distance, i) for i in devices if i - distance in devices]
    return lax.ppermute(block, axis, route)


def lane_pairs(bands):
    levels = bands.shape[-1]
    low = jnp.pad(bands[:8], ((0, 0), (0, 0), (0, LANES - levels)))
    high = jnp.pad(bands[8:], ((0, 1), (0, 0), (64, 64 - levels)))
    return low + high


def to_edges(slab, axis):
    size = lax.axis_size(axis)
    t = jnp.transpose(slab, (0, 1, 3, 4, 2))
    first = lane_pairs(t[0].reshape(15, *t.shape[3:]))
    last = lane_pairs(t[1, :, ::-1].reshape(15, *t.shape[3:]))
    zero = jnp.zeros((size - 2, *first.shape), first.dtype)
    sent = jnp.concatenate([first[None], zero, last[None]], axis=0)
    return lax.all_to_all(sent, axis, 0, 0, tiled=True)


def iota8(dim):
    return lax.broadcasted_iota(jnp.int32, (8, LANES), dim)


def axis_ends(axis):
    at = lax.axis_index(axis)
    return at == 0, at == lax.axis_size(axis) - 1


def loop(count, unroll, body, carry):
    assert count % unroll == 0

    def trip(g, carry):
        for i in range(unroll):
            carry = body(g * unroll + i, carry)
        return carry

    return lax.fori_loop(0, count // unroll, trip, carry)


def each(count, unroll, body):
    def step(i, carry):
        body(i)
        return carry

    loop(count, unroll, step, 0)


def side_bands(sn_w, sng, sn_e, bs, shift):
    zero = jnp.zeros((8, LANES), jnp.float32)
    spare = jnp.zeros((LANES - 24 - sng.shape[1], LANES), jnp.float32)

    def clear(i):
        for k in range(3):
            bs[k, pl.ds(pl.multiple_of(i * 8, 8), 8), :] = zero

    each(64, 4, clear)
    for s in range(8):
        b = jnp.concatenate([zero, sn_w[s], sng[s], sn_e[s], spare], axis=0).T
        for half in range(2):
            kj = s + 8 * half
            if kj < 15:
                bs[kj // 5, pl.ds(kj % 5 + shift, 64, stride=8), :] = b[64 * half : 64 * half + 64]


def on_sides(body):
    for north, is_edge in enumerate(axis_ends("gy")):

        @pl.when(is_edge)
        def _():
            body(north)


def turned(parts):
    zero = jnp.zeros((8, LANES), jnp.float32)
    rows = [zero] + parts + [zero] * (LANES // 8 - 1 - len(parts))
    return jnp.concatenate(rows, axis=0).T


def fill_rates(rate_, width, from_w, from_e):
    levels, size_x = from_w.shape[0] - 1, width.shape[0]
    rate_[2:8, :] = from_w[levels, HALO : 2 * HALO, :]
    rate_[8 : 8 + size_x, :] = width[...].astype(jnp.float32)
    rate_[8 + size_x : 14 + size_x, :] = from_e[levels, HALO : 2 * HALO, :]


def factors(coefs, dst, at):
    def body(z, prev):
        new = []
        for s, m in zip(at, prev):
            r = coefs[s : s + 8, :]
            m = 1.0 / (1.0 + 2.0 * r - r * r * m)
            dst[z, s : s + 8, :] = m
            new.append(m)
        return tuple(new)

    zero = jnp.zeros((8, LANES), jnp.float32)
    lax.fori_loop(0, dst.shape[0], body, tuple(zero for _ in at))


def fill_coefs(R_, coef, halo_r):
    size_x = coef.shape[0]
    R_[OFF : OFF + size_x, :] = coef[...]
    R_[OFF - 8 : OFF, :] = halo_r[0:8, :]
    R_[OFF + size_x : OFF + size_x + 8, :] = halo_r[8:16, :]


def end_bands(weg, cw, ce):
    groups = weg.shape[0]
    zero = jnp.zeros((8, LANES), jnp.float32)

    def clear(i):
        for k in range(3):
            cw[k, pl.ds(pl.multiple_of(i * 8, 8), 8), :] = zero
            ce[k, pl.ds(pl.multiple_of(i * 8, 8), 8), :] = zero

    each(64, 4, clear)
    for s in range(8):
        a = jnp.concatenate([weg[g, s] for g in range(groups)], axis=0).T
        for half in range(2):
            kj = s + 8 * half
            if kj < 15:
                k, j = kj // 5, kj % 5
                cw[k, pl.ds(j, 64, stride=8), :] = a[64 * half : 64 * half + 64]
                ce[k, pl.ds(3 + j, 64, stride=8), :] = a[64 * half : 64 * half + 64]


def rim_kernel(p, u, v, w, coef, width, east, west, held, held_c, held_w, sems):
    levels, size_x, _ = u.shape
    zero = jnp.zeros((8, LANES), jnp.float32)
    copies = []
    for f, src in enumerate((p, u, v, w)):
        for side, lo in enumerate((size_x - 8, 0)):
            copies.append(pltpu.make_async_copy(src.at[:, lo : lo + 8, :], held.at[side, f], sems.at[side, f]))
    for side, lo in enumerate((size_x - 8, 0)):
        copies.append(pltpu.make_async_copy(coef.at[lo : lo + 8, :], held_c.at[side], sems.at[side, 4]))
        copies.append(pltpu.make_async_copy(width.at[lo : lo + 8, :], held_w.at[side], sems.at[side, 5]))
    for copy in copies:
        copy.start()
    for copy in copies:
        copy.wait()
    for side, (msg, at) in enumerate(((east, slice(8 - HALO, 8)), (west, slice(0, HALO)))):
        for b in range(3):
            msg[levels, 8 * b : 8 * b + 8, :] = zero
        msg[levels, 0:HALO, :] = held_c[side, at, :]
        msg[levels, HALO : 2 * HALO, :] = held_w[side, at, :].astype(jnp.float32)

    def pack(z):
        for f in range(4):
            east[z, HALO * f : HALO * f + HALO, :] = held[0, f, z, 8 - HALO : 8, :]
            west[z, HALO * f : HALO * f + HALO, :] = held[1, f, z, 0:HALO, :]

    each(levels, 4, pack)


def strip_kernel(
    nx, p, u, v, w, coef, width, weg, sn_w, sng, sn_e, from_w, from_e,
    px, ux, vx, wx, halo_r, own, own_r, north, south,
    cw, ce, bs, rate_, sems,
):
    levels, size_x, _ = u.shape
    blocks = size_x // 8
    starts = [OFF - 8 + 8 * b for b in range(blocks + 2)]
    ends_at = (OFF, OFF + size_x - 8)
    zero = jnp.zeros((8, LANES), jnp.float32)
    is_west, is_east = axis_ends("gx")
    fields = ((p, px, 2), (u, ux, 0), (v, vx, 1), (w, wx, None))
    copies = [
        pltpu.make_async_copy(src, dst.at[:, OFF : OFF + size_x, :], sems.at[f])
        for f, (src, dst, _) in enumerate(fields)
    ]
    for copy in copies:
        copy.start()

    for f, (_, dst, _) in enumerate(fields):

        def unpack(z):
            dst[z, OFF - HALO : OFF, :] = from_w[z, HALO * f : HALO * f + HALO, :]
            dst[z, OFF + size_x : OFF + size_x + HALO, :] = from_e[z, HALO * f : HALO * f + HALO, :]

        each(levels, 6, unpack)
    halo_r[2:8, :] = from_w[levels, 0:HALO, :]
    halo_r[8:14, :] = from_e[levels, 0:HALO, :]

    @pl.when(is_west | is_east)
    def _():
        end_bands(weg, cw, ce)

    on_sides(lambda north: side_bands(sn_w, sng, sn_e, bs, 3 * north))
    fill_rates(rate_, width, from_w, from_e)

    def ends(dst, k):
        x = iota8(0).astype(jnp.float32) + (lax.axis_index("gx") * size_x).astype(jnp.float32)
        rate_w = width[0:8, :].astype(jnp.float32)
        rate_e = width[size_x - 8 : size_x, :].astype(jnp.float32)
        weight_w = jnp.maximum(rate_w - x, 0.0) / rate_w
        weight_e = jnp.maximum(rate_e - ((nx - 1.0) - (x + (size_x - 8.0))), 0.0) / rate_e

        def body(z):
            rows = pl.ds(pl.multiple_of(z * 8, 8), 8)
            for at, weight, band in zip(ends_at, (weight_w, weight_e), (cw, ce)):
                val = dst[z, at : at + 8, :]
                dst[z, at : at + 8, :] = val + weight * (band[k, rows, :] - val)

        each(levels, 6, body)

    lane_group = iota8(1) // 16

    for f, (_, dst, k) in enumerate(fields):
        copies[f].wait()
        if k is not None:

            @pl.when(is_west | is_east)
            def _():
                ends(dst, k)

        def group(g, _):
            acc = None
            for zi in range(ZG):
                z = g * ZG + zi
                parts = [dst[z, s : s + 8, :] for s in starts]
                if k is None:
                    parts = [2.0 * part for part in parts]
                    for s, part in zip(starts, parts):
                        dst[z, s : s + 8, :] = part
                parts = [pltpu.roll(part, (8 + 16 * zi) % LANES, 1) for part in parts]
                if acc is None:
                    acc = parts
                else:
                    acc = [jnp.where(lane_group == zi, part, old) for part, old in zip(parts, acc)]
            t = turned(acc)
            for zi in range(ZG):
                z = g * ZG + zi
                both = t[16 * zi : 16 * zi + 16]
                own[f, z] = both
                north[z, HALO * f : HALO * f + HALO, :] = both[2:8]
                south[z, HALO * f : HALO * f + HALO, :] = both[8:14]
            return 0

        lax.fori_loop(0, levels // ZG, group, 0, unroll=2)

    def blend(north):
        rate = turned([pltpu.roll(rate_[8 * b : 8 * b + 8, :], 8, 1) for b in range(blocks + 2)])
        at = slice(0, 8) if north else slice(8, 16)
        y = iota8(0).astype(jnp.float32)
        rate = jnp.maximum(rate[at], 1.0)
        weight = jnp.maximum(rate - (7.0 - y if north else y), 0.0) / rate

        def body(z):
            rows = pl.ds(pl.multiple_of(z * 8, 8), 8)
            for f, (_, _, k) in enumerate(fields[:3]):
                val = own[f, z, at, :]
                own[f, z, at, :] = val + weight * (bs[k, rows, :] - val)

        each(levels, 6, body)

    on_sides(blend)

    parts = [halo_r[0:8, :]]
    parts += [coef[8 * b : 8 * b + 8, :] for b in range(blocks)]
    parts += [halo_r[8:16, :]]
    t = turned([pltpu.roll(part, 8, 1) for part in parts])
    own_r[...] = t[0:16]
    for msg in (north, south):
        for b in range(3):
            msg[levels, 8 * b : 8 * b + 8, :] = zero
    north[levels, 0:HALO, :] = t[2:8]
    south[levels, 0:HALO, :] = t[8:14]


def prep_kernel(
    px, ux, vx, coef, halo_r, width, from_w, from_e, sn_w, sng, sn_e,
    pb, ub, vb, E_, M_,
    bs, bt, rate_, R_,
):
    levels, _, _ = px.shape
    blocks = width.shape[0] // 8
    starts = [OFF - 8 + 8 * b for b in range(blocks + 2)]
    fields = ((px, pb, 2), (ux, ub, 0), (vx, vb, 1))

    def take(z):
        for src, dst, _ in fields:
            for s in starts:
                dst[z, s : s + 8, :] = src[z, s : s + 8, :]

    each(levels, 2, take)

    def blend(north):
        side_bands(sn_w, sng, sn_e, bs, 3 * north)
        for k in range(3):
            for g in range(4):
                bt[k, g] = bs[k, g * LANES : (g + 1) * LANES, :].T
        fill_rates(rate_, width, from_w, from_e)
        y = iota8(1).astype(jnp.float32)
        dist = 127.0 - y if north else y
        for first in range(0, blocks + 2, SB):
            some = range(first, min(first + SB, blocks + 2))
            weights = []
            for b in some:
                rate = jnp.maximum(rate_[8 * b : 8 * b + 8, :], 1.0)
                weights.append(jnp.maximum(rate - dist, 0.0) / rate)

            def trip(g, _):
                for _, dst, k in fields:
                    for i in range(ZS):
                        z = g * ZS + i
                        shift = lax.rem(LANES + 120 * north - 8 * lax.rem(z, 16), LANES)
                        for b, weight in zip(some, weights):
                            s = starts[b]
                            band = pltpu.roll(bt[k, z // 16, s : s + 8, :], shift, 1)
                            val = dst[z, s : s + 8, :]
                            dst[z, s : s + 8, :] = val + weight * (band - val)
                return 0

            lax.fori_loop(0, levels // ZS, trip, 0)

    on_sides(blend)
    lane0 = iota8(1) == 0

    def diverge(z):
        for s in starts:
            u = ub[z, s : s + 8, :]
            u_w = ub[z, s - 1 : s + 7, :]
            v = vb[z, s : s + 8, :]
            v_s = jnp.where(lane0, 0.0, pltpu.roll(v, 1, 1))
            E_[z, s : s + 8, :] = SPREAD * ((u - u_w) + (v - v_s))

    each(levels, 6, diverge)
    fill_coefs(R_, coef, halo_r)
    factors(R_, M_, starts)


def step_kernel(
    p0, u0, v0, w0, e0, M_, coef, halo_r, own, own_r, from_s, from_n,
    u_out, v_out, w_out, p_out,
    P_, E_, W_, S_, Q_, D_, R_, sP, sE, sW, sQ, sM, sR, rows, T_, sems,
):
    levels, size_x, _ = u_out.shape
    blocks = size_x // 8
    starts = [8 * b for b in range(1, blocks + 3)]
    main = [OFF + 8 * b for b in range(blocks)]
    ahead = starts[::2]
    sstarts = [SROW, SROW + 8, NROW, NROW + 8]
    zero = jnp.zeros((8, LANES), jnp.float32)
    sub = iota8(0)
    lane = iota8(1)
    is_west, is_east = axis_ends("gx")
    is_south, is_north = axis_ends("gy")
    mask_w = (sub == 0) & is_west
    mask_e = (sub == 7) & is_east
    smask_w = (lane == OFF) & is_west
    smask_e = (lane == OFF + size_x - 1) & is_east
    smask_s = (sub == 0) & is_south
    smask_n = (sub == 7) & is_north
    lane0 = lane == 0
    lane127 = lane == LANES - 1
    AB = ACCEL * SPREAD

    def unpack(z):
        for f, dst in enumerate((sP, sQ, sM, sW)):
            lo = HALO * f
            dst[z, SROW + 8 : SROW + 16, :] = own[f, z, 8:16, :]
            dst[z, NROW : NROW + 8, :] = own[f, z, 0:8, :]
            dst[z, SROW + 8 - HALO : SROW + 8, :] = from_s[z, lo : lo + HALO, :]
            dst[z, NROW + 8 : NROW + 8 + HALO, :] = from_n[z, lo : lo + HALO, :]

    each(levels, 2, unpack)
    fill_coefs(R_, coef, halo_r)
    sR[SROW + 8 : SROW + 16, :] = own_r[8:16, :]
    sR[NROW : NROW + 8, :] = own_r[0:8, :]
    sR[SROW + 8 - HALO : SROW + 8, :] = from_s[levels, 0:HALO, :]
    sR[NROW + 8 : NROW + 8 + HALO, :] = from_n[levels, 0:HALO, :]

    def strip_init(z):
        for s in sstarts:
            u = sQ[z, s : s + 8, :]
            v = sM[z, s : s + 8, :]
            v_s = sM[z, s - 1 : s + 7, :]
            sE[z, s : s + 8, :] = SPREAD * ((u - pltpu.roll(u, 1, 1)) + (v - v_s))
        rows[SUBSTEPS, pl.ds(2 * z, 1), :] = sM[z, SROW + 7 : SROW + 8, :]

    each(levels, 6, strip_init)

    factors(sR, sM, sstarts)

    def descend(qq, ww, mm, rr, at, sectioned, size, old=None):
        given = ww if old is None else old

        def down(z, qs, ds, last=False):
            new = []
            qn = None if last else [qq[z + 1, s : s + 8, :] for s in at]
            for i, s in enumerate(at):
                rhs = given[z, s : s + 8, :] + (qs[i] if last else qs[i] - qn[i])
                if ds is not None:
                    rhs = rhs + rr[s : s + 8, :] * ds[i]
                d = mm[z, s : s + 8, :] * rhs
                ww[z, s : s + 8, :] = d
                new.append(d)
            return qn, tuple(new)

        groups = levels // size
        for i in range(2 * size):
            sectioned(i)
        qs = [qq[0, s : s + 8, :] for s in at]
        ds = None
        for i in range(size - 1):
            qs, ds = down(i, qs, ds)

        def fwd(g, ds):
            qs = [qq[g * size - 1, s : s + 8, :] for s in at]
            for i in range(size):
                qs, ds = down(g * size - 1 + i, qs, ds)
            for i in range(size):
                sectioned((g + 1) * size + i)
            return ds

        ds = lax.fori_loop(1, groups - 1, fwd, ds)
        first = (groups - 1) * size - 1
        qs = [qq[first, s : s + 8, :] for s in at]
        for i in range(size):
            qs, ds = down(first + i, qs, ds)
        return down(levels - 1, qs, ds, last=True)[1]

    def ascend(pp, qq, ww, mm, rr, at, ws, size, scale=1.0, done=None, also=None):
        def up(z, ws):
            new = []
            if also:
                also(z)
            for j, s in enumerate(at):
                w = ww[z, s : s + 8, :] + mm[z, s : s + 8, :] * (rr[s : s + 8, :] * ws[j])
                ww[z, s : s + 8, :] = w if scale == 1.0 else scale * w
                pp[z + 1, s : s + 8, :] = qq[z + 1, s : s + 8, :] - 0.25 * (ws[j] - w)
                new.append(w)
            return tuple(new)

        chunk = levels // 4 if done else levels
        if also:
            also(levels - 1)
        if scale != 1.0:
            for j, s in enumerate(at):
                ww[levels - 1, s : s + 8, :] = scale * ws[j]
        for hi in range(levels, 0, -chunk):
            top = hi - 1
            left = chunk
            if hi == levels:
                for i in range(size - 1):
                    ws = up(levels - 2 - i, ws)
                top = levels - 1 - size
                left = chunk - size

            def bwd(g, ws):
                for i in range(size):
                    ws = up(top - g * size - i, ws)
                return ws

            ws = lax.fori_loop(0, left // size, bwd, ws)
            if hi == chunk:
                for j, s in enumerate(at):
                    pp[0, s : s + 8, :] = qq[0, s : s + 8, :] - 0.25 * ws[j]
            if done:
                done(hi - chunk, hi)

    def strip_step(k, _):
        def sectioned(z):
            for s in sstarts:
                p = sP[z, s : s + 8, :]
                p_s = sP[z, s - 1 : s + 7, :]
                p_n = sP[z, s + 1 : s + 9, :]
                p_w = jnp.where(smask_w, p, pltpu.roll(p, 1, 1))
                p_e = jnp.where(smask_e, 0.0, pltpu.roll(p, LANES - 1, 1))
                if s == SROW + 8:
                    p_s = jnp.where(smask_s, p, p_s)
                if s == NROW:
                    p_n = jnp.where(smask_n, 0.0, p_n)
                e = sE[z, s : s + 8, :] - AB * (((p_w + p_e) + (p_s + p_n)) - 4.0 * p)
                sE[z, s : s + 8, :] = e
                sQ[z, s : s + 8, :] = p - e
            edge_s = jnp.where(is_south, sP[z, SROW + 8 : SROW + 9, :], sP[z, SROW + 7 : SROW + 8, :])
            edge_n = jnp.where(is_north, 0.0, sP[z, NROW + 8 : NROW + 9, :])
            rows[k, pl.ds(2 * z, 1), :] = edge_s
            rows[k, pl.ds(lax.rem(2 * z + LANES - 1, LANES), 1), :] = edge_n

        ws = descend(sQ, sW, sM, sR, sstarts, sectioned, SU)
        ascend(sP, sQ, sW, sM, sR, sstarts, ws, 6)
        return 0

    lax.fori_loop(0, SUBSTEPS, strip_step, 0)

    for k in range(SUBSTEPS + 1):
        T_[k] = rows[k].T

    def edges(k, z, s):
        return pltpu.roll(T_[k, s : s + 8, :], lax.rem(2 * LANES - 2 * z, LANES), 1)

    def main_down(k, first=False):
        def sectioned(z):
            pp = p0 if first else P_
            for s in starts:
                p = pp[z, s : s + 8, :]
                p_w = pp[z, s - 1 : s + 7, :]
                p_e = pp[z, s + 1 : s + 9, :]
                if s == main[0]:
                    p_w = jnp.where(mask_w, p, p_w)
                if s == main[-1]:
                    p_e = jnp.where(mask_e, 0.0, p_e)
                edge = edges(0, z, s) if first else D_[z, s : s + 8, :] if s in ahead else edges(k, z, s)
                p_s = jnp.where(lane0, edge, pltpu.roll(p, 1, 1))
                p_n = jnp.where(lane127, edge, pltpu.roll(p, LANES - 1, 1))
                if first:
                    e = e0[z, s : s + 8, :] - jnp.where(lane0, SPREAD * edges(SUBSTEPS, z, s), 0.0)
                else:
                    e = E_[z, s : s + 8, :]
                e = e - AB * (((p_w + p_e) + (p_s + p_n)) - 4.0 * p)
                E_[z, s : s + 8, :] = e
                if s != starts[0]:
                    S_[z, s : s + 8, :] = p if first else S_[z, s : s + 8, :] + p
                Q_[z, s : s + 8, :] = p - e

        return descend(Q_, W_, M_, R_, starts, sectioned, FU if first else MU, w0 if first else None)

    def main_up(k, ws):
        def also(z):
            for s in ahead:
                D_[z, s : s + 8, :] = edges(k + 1, z, s)

        ascend(P_, Q_, W_, M_, R_, starts, ws, MB, also=also)

    def main_step(k, _):
        main_up(k, main_down(k))
        return 0

    main_up(0, main_down(0, True))
    lax.fori_loop(1, SUBSTEPS - 1, main_step, 0)
    ws = main_down(SUBSTEPS - 1)

    total = T_[0]
    for k in range(1, SUBSTEPS):
        total = total + T_[k]
    T_[0] = total

    chunk = levels // 4
    copies = []

    def send(src, dst, lo, hi):
        at = slice(OFF, OFF + size_x)
        copy = pltpu.make_async_copy(src.at[lo:hi, at, :], dst.at[lo:hi], sems.at[len(copies)])
        copy.start()
        copies.append(copy)

    def finish(z):
        for s in main:
            total = S_[z, s : s + 8, :]
            east = S_[z, s + 1 : s + 9, :]
            if s == main[-1]:
                east = jnp.where(mask_e, 0.0, east)
            north = jnp.where(lane127, edges(0, z, s), pltpu.roll(total, LANES - 1, 1))
            E_[z, s : s + 8, :] = u0[z, s : s + 8, :] - ACCEL * (east - total)
            S_[z, s : s + 8, :] = v0[z, s : s + 8, :] - ACCEL * (north - total)

    for c in range(4):
        each(chunk, chunk if chunk < 5 else 5, lambda i: finish(c * chunk + i))
        send(E_, u_out, c * chunk, (c + 1) * chunk)
        send(S_, v_out, c * chunk, (c + 1) * chunk)

    def done(lo, hi):
        send(W_, w_out, lo, hi)
        send(P_, p_out, lo + 1 if lo else 0, min(hi + 1, levels))

    ascend(P_, Q_, W_, M_, R_, main, ws[1 : 1 + blocks], chunk if chunk < 5 else 5, 0.5, done)
    for copy in copies:
        copy.wait()


def whole(u_wind, v_wind, w_wind, pressure, vert_coef, we_slab, sn_slab, relax_width):
    levels, size_x, _ = pressure.shape
    stay = [pltpu.with_memory_space_constraint(x, pltpu.HBM) for x in (pressure, u_wind, v_wind, w_wind, vert_coef, relax_width)]
    nx = float(size_x * lax.axis_size("gx"))
    f32 = jnp.float32
    block = jax.ShapeDtypeStruct(pressure.shape, f32)
    message = jax.ShapeDtypeStruct((levels + 1, 4 * HALO, LANES), f32)
    ext = size_x + 2 * OFF
    extended = jax.ShapeDtypeStruct((levels, ext, LANES), f32)

    east, west = pl.pallas_call(
        rim_kernel,
        out_shape=(message, message),
        in_specs=[HBM] * 6,
        out_specs=[VMEM] * 2,
        scratch_shapes=[
            pltpu.VMEM((2, 4, levels, 8, LANES), f32),
            pltpu.VMEM((2, 8, LANES), f32),
            pltpu.VMEM((2, 8, LANES), jnp.int32),
            pltpu.SemaphoreType.DMA((2, 6)),
        ],
        compiler_params=pltpu.CompilerParams(vmem_limit_bytes=24 << 20),
        name="rims",
    )(*stay)
    sn_slab, we_slab, east, west = lax.optimization_barrier((sn_slab, we_slab, east, west))
    from_w = passed_along(east, "gx", 1)
    from_e = passed_along(west, "gx", -1)

    sng = to_edges(sn_slab, "gy")
    sng = jnp.transpose(sng, (1, 0, 2, 3)).reshape(8, size_x, LANES)
    sn_w = passed_along(sng[:, size_x - 8 :], "gx", 1)
    sn_e = passed_along(sng[:, :8], "gx", -1)
    weg = to_edges(we_slab, "gx")

    bands = pltpu.VMEM((3, 512, LANES), f32)
    px, ux, vx, wx, halo_r, own, own_r, north, south = pl.pallas_call(
        lambda *refs: strip_kernel(nx, *refs),
        out_shape=(
            extended,
            extended,
            extended,
            extended,
            jax.ShapeDtypeStruct((16, LANES), f32),
            jax.ShapeDtypeStruct((4, levels, 16, LANES), f32),
            jax.ShapeDtypeStruct((16, LANES), f32),
            message,
            message,
        ),
        in_specs=[HBM] * 4 + [VMEM] * 8,
        out_specs=[VMEM] * 9,
        scratch_shapes=[
            bands,
            bands,
            bands,
            pltpu.VMEM((size_x + 16, LANES), f32),
            pltpu.SemaphoreType.DMA((4,)),
        ],
        compiler_params=pltpu.CompilerParams(vmem_limit_bytes=8 << 20),
        name="strips",
    )(*stay[:4], vert_coef, relax_width, weg, sn_w, sng, sn_e, from_w, from_e)
    from_s = passed_along(north, "gy", 1)
    from_n = passed_along(south, "gy", -1)
    pb, ub, vb, e0, m0 = pl.pallas_call(
        prep_kernel,
        out_shape=(extended,) * 5,
        in_specs=[VMEM] * 11,
        out_specs=[VMEM] * 5,
        scratch_shapes=[
            bands,
            pltpu.VMEM((3, 4, LANES, LANES), f32),
            pltpu.VMEM((size_x + 16, LANES), f32),
            pltpu.VMEM((ext, LANES), f32),
        ],
        compiler_params=pltpu.CompilerParams(vmem_limit_bytes=6 << 20),
        cost_estimate=pl.CostEstimate(flops=20_000_000, bytes_accessed=20_000_000, transcendentals=0),
        name="prep",
    )(px, ux, vx, vert_coef, halo_r, relax_width, from_w, from_e, sn_w, sng, sn_e)

    big = pltpu.VMEM((levels, ext, LANES), f32)
    strip = pltpu.VMEM((levels, SROWS, LANES), f32)
    return pl.pallas_call(
        step_kernel,
        out_shape=(block, block, block, block),
        in_specs=[VMEM] * 12,
        out_specs=[HBM] * 4,
        scratch_shapes=[big] * 6
        + [pltpu.VMEM((ext, LANES), f32)]
        + [strip] * 5
        + [
            pltpu.VMEM((SROWS, LANES), f32),
            pltpu.VMEM((SUBSTEPS + 1, LANES, LANES), f32),
            pltpu.VMEM((SUBSTEPS + 1, LANES, LANES), f32),
            pltpu.SemaphoreType.DMA((16,)),
        ],
        compiler_params=pltpu.CompilerParams(vmem_limit_bytes=30 << 20),
        name="substeps",
    )(pb, ub, vb, wx, e0, m0, vert_coef, halo_r, own, own_r, from_s, from_n)


def solution(mesh):
    placed = (
        P(None, "gx", "gy"),
        P(None, "gx", "gy"),
        P(None, "gx", "gy"),
        P(None, "gx", "gy"),
        P("gx", "gy"),
        P(None, None, None, None, ("gy", "gx")),
        P(None, None, None, None, ("gx", "gy")),
        P("gx", "gy"),
    )
    return jax.shard_map(
        whole,
        mesh=mesh,
        in_specs=placed,
        out_specs=(P(None, "gx", "gy"),) * 4,
        check_vma=False,
    )
```

```python
import jax
import jax.numpy as jnp
from jax import lax
from jax.experimental import pallas as pl
from jax.experimental.pallas import tpu as pltpu
from jax.sharding import PartitionSpec as P


SUBSTEPS = 6
HALO = 6
OFF = 16
ZG = 6
SB = 5
ZS = 12
LANES = 128
ACCEL = 0.3
SPREAD = 0.3
SROW = 8
NROW = 24
SROWS = 48
MU = 15
FU = 10
MB = 20
SU = 20

VMEM = pl.BlockSpec(memory_space=pltpu.VMEM)
HBM = pl.BlockSpec(memory_space=pltpu.HBM)


def passed_along(block, axis, distance):
    devices = range(lax.axis_size(axis))
    route = [(i - distance, i) for i in devices if i - distance in devices]
    return lax.ppermute(block, axis, route)


def lane_pairs(bands):
    levels = bands.shape[-1]
    low = jnp.pad(bands[:8], ((0, 0), (0, 0), (0, LANES - levels)))
    high = jnp.pad(bands[8:], ((0, 1), (0, 0), (64, 64 - levels)))
    return low + high


def to_edges(slab, axis):
    size = lax.axis_size(axis)
    t = jnp.transpose(slab, (0, 1, 3, 4, 2))
    first = lane_pairs(t[0].reshape(15, *t.shape[3:]))
    last = lane_pairs(t[1, :, ::-1].reshape(15, *t.shape[3:]))
    zero = jnp.zeros((size - 2, *first.shape), first.dtype)
    sent = jnp.concatenate([first[None], zero, last[None]], axis=0)
    return lax.all_to_all(sent, axis, 0, 0, tiled=True)


def iota8(dim):
    return lax.broadcasted_iota(jnp.int32, (8, LANES), dim)


def axis_ends(axis):
    at = lax.axis_index(axis)
    return at == 0, at == lax.axis_size(axis) - 1


def loop(count, unroll, body, carry):
    assert count % unroll == 0

    def trip(g, carry):
        for i in range(unroll):
            carry = body(g * unroll + i, carry)
        return carry

    return lax.fori_loop(0, count // unroll, trip, carry)


def each(count, unroll, body):
    def step(i, carry):
        body(i)
        return carry

    loop(count, unroll, step, 0)


def side_bands(sn_w, sng, sn_e, bs, shift):
    zero = jnp.zeros((8, LANES), jnp.float32)
    spare = jnp.zeros((LANES - 24 - sng.shape[1], LANES), jnp.float32)

    def clear(i):
        for k in range(3):
            bs[k, pl.ds(pl.multiple_of(i * 8, 8), 8), :] = zero

    each(64, 4, clear)
    for s in range(8):
        b = jnp.concatenate([zero, sn_w[s], sng[s], sn_e[s], spare], axis=0).T
        for half in range(2):
            kj = s + 8 * half
            if kj < 15:
                bs[kj // 5, pl.ds(kj % 5 + shift, 64, stride=8), :] = b[64 * half : 64 * half + 64]


def on_sides(body):
    for north, is_edge in enumerate(axis_ends("gy")):

        @pl.when(is_edge)
        def _():
            body(north)


def turned(parts):
    zero = jnp.zeros((8, LANES), jnp.float32)
    rows = [zero] + parts + [zero] * (LANES // 8 - 1 - len(parts))
    return jnp.concatenate(rows, axis=0).T


def fill_rates(rate_, width, from_w, from_e):
    levels, size_x = from_w.shape[0] - 1, width.shape[0]
    rate_[2:8, :] = from_w[levels, HALO : 2 * HALO, :]
    rate_[8 : 8 + size_x, :] = width[...].astype(jnp.float32)
    rate_[8 + size_x : 14 + size_x, :] = from_e[levels, HALO : 2 * HALO, :]


def factors(coefs, dst, at):
    def body(z, prev):
        new = []
        for s, m in zip(at, prev):
            r = coefs[s : s + 8, :]
            m = 1.0 / (1.0 + 2.0 * r - r * r * m)
            dst[z, s : s + 8, :] = m
            new.append(m)
        return tuple(new)

    zero = jnp.zeros((8, LANES), jnp.float32)
    lax.fori_loop(0, dst.shape[0], body, tuple(zero for _ in at))


def fill_coefs(R_, coef, halo_r):
    size_x = coef.shape[0]
    R_[OFF : OFF + size_x, :] = coef[...]
    R_[OFF - 8 : OFF, :] = halo_r[0:8, :]
    R_[OFF + size_x : OFF + size_x + 8, :] = halo_r[8:16, :]


def end_bands(weg, cw, ce):
    groups = weg.shape[0]
    zero = jnp.zeros((8, LANES), jnp.float32)

    def clear(i):
        for k in range(3):
            cw[k, pl.ds(pl.multiple_of(i * 8, 8), 8), :] = zero
            ce[k, pl.ds(pl.multiple_of(i * 8, 8), 8), :] = zero

    each(64, 4, clear)
    for s in range(8):
        a = jnp.concatenate([weg[g, s] for g in range(groups)], axis=0).T
        for half in range(2):
            kj = s + 8 * half
            if kj < 15:
                k, j = kj // 5, kj % 5
                cw[k, pl.ds(j, 64, stride=8), :] = a[64 * half : 64 * half + 64]
                ce[k, pl.ds(3 + j, 64, stride=8), :] = a[64 * half : 64 * half + 64]


def rim_kernel(p, u, v, w, coef, width, east, west, held, held_c, held_w, sems):
    levels, size_x, _ = u.shape
    zero = jnp.zeros((8, LANES), jnp.float32)
    copies = []
    for f, src in enumerate((p, u, v, w)):
        for side, lo in enumerate((size_x - 8, 0)):
            copies.append(pltpu.make_async_copy(src.at[:, lo : lo + 8, :], held.at[side, f], sems.at[side, f]))
    for side, lo in enumerate((size_x - 8, 0)):
        copies.append(pltpu.make_async_copy(coef.at[lo : lo + 8, :], held_c.at[side], sems.at[side, 4]))
        copies.append(pltpu.make_async_copy(width.at[lo : lo + 8, :], held_w.at[side], sems.at[side, 5]))
    for copy in copies:
        copy.start()
    for copy in copies:
        copy.wait()
    for side, (msg, at) in enumerate(((east, slice(8 - HALO, 8)), (west, slice(0, HALO)))):
        for b in range(3):
            msg[levels, 8 * b : 8 * b + 8, :] = zero
        msg[levels, 0:HALO, :] = held_c[side, at, :]
        msg[levels, HALO : 2 * HALO, :] = held_w[side, at, :].astype(jnp.float32)

    def pack(z):
        for f in range(4):
            east[z, HALO * f : HALO * f + HALO, :] = held[0, f, z, 8 - HALO : 8, :]
            west[z, HALO * f : HALO * f + HALO, :] = held[1, f, z, 0:HALO, :]

    each(levels, 4, pack)


def strip_kernel(
    nx, p, u, v, w, coef, width, weg, sn_w, sng, sn_e, from_w, from_e,
    px, ux, vx, wx, halo_r, own, own_r, north, south,
    cw, ce, bs, rate_, sems,
):
    levels, size_x, _ = u.shape
    blocks = size_x // 8
    starts = [OFF - 8 + 8 * b for b in range(blocks + 2)]
    ends_at = (OFF, OFF + size_x - 8)
    zero = jnp.zeros((8, LANES), jnp.float32)
    is_west, is_east = axis_ends("gx")
    fields = ((p, px, 2), (u, ux, 0), (v, vx, 1), (w, wx, None))
    copies = [
        pltpu.make_async_copy(src, dst.at[:, OFF : OFF + size_x, :], sems.at[f])
        for f, (src, dst, _) in enumerate(fields)
    ]
    for copy in copies:
        copy.start()

    for f, (_, dst, _) in enumerate(fields):

        def unpack(z):
            dst[z, OFF - HALO : OFF, :] = from_w[z, HALO * f : HALO * f + HALO, :]
            dst[z, OFF + size_x : OFF + size_x + HALO, :] = from_e[z, HALO * f : HALO * f + HALO, :]

        each(levels, 6, unpack)
    halo_r[2:8, :] = from_w[levels, 0:HALO, :]
    halo_r[8:14, :] = from_e[levels, 0:HALO, :]

    @pl.when(is_west | is_east)
    def _():
        end_bands(weg, cw, ce)

    on_sides(lambda north: side_bands(sn_w, sng, sn_e, bs, 3 * north))
    fill_rates(rate_, width, from_w, from_e)

    def ends(dst, k):
        x = iota8(0).astype(jnp.float32) + (lax.axis_index("gx") * size_x).astype(jnp.float32)
        rate_w = width[0:8, :].astype(jnp.float32)
        rate_e = width[size_x - 8 : size_x, :].astype(jnp.float32)
        weight_w = jnp.maximum(rate_w - x, 0.0) / rate_w
        weight_e = jnp.maximum(rate_e - ((nx - 1.0) - (x + (size_x - 8.0))), 0.0) / rate_e

        def body(z):
            rows = pl.ds(pl.multiple_of(z * 8, 8), 8)
            for at, weight, band in zip(ends_at, (weight_w, weight_e), (cw, ce)):
                val = dst[z, at : at + 8, :]
                dst[z, at : at + 8, :] = val + weight * (band[k, rows, :] - val)

        each(levels, 6, body)

    lane_group = iota8(1) // 16

    for f, (_, dst, k) in enumerate(fields):
        copies[f].wait()
        if k is not None:

            @pl.when(is_west | is_east)
            def _():
                ends(dst, k)

        def group(g, _):
            acc = None
            for zi in range(ZG):
                z = g * ZG + zi
                parts = [dst[z, s : s + 8, :] for s in starts]
                if k is None:
                    parts = [2.0 * part for part in parts]
                    for s, part in zip(starts, parts):
                        dst[z, s : s + 8, :] = part
                parts = [pltpu.roll(part, (8 + 16 * zi) % LANES, 1) for part in parts]
                if acc is None:
                    acc = parts
                else:
                    acc = [jnp.where(lane_group == zi, part, old) for part, old in zip(parts, acc)]
            t = turned(acc)
            for zi in range(ZG):
                z = g * ZG + zi
                both = t[16 * zi : 16 * zi + 16]
                own[f, z] = both
                north[z, HALO * f : HALO * f + HALO, :] = both[2:8]
                south[z, HALO * f : HALO * f + HALO, :] = both[8:14]
            return 0

        lax.fori_loop(0, levels // ZG, group, 0, unroll=2)

    def blend(north):
        rate = turned([pltpu.roll(rate_[8 * b : 8 * b + 8, :], 8, 1) for b in range(blocks + 2)])
        at = slice(0, 8) if north else slice(8, 16)
        y = iota8(0).astype(jnp.float32)
        rate = jnp.maximum(rate[at], 1.0)
        weight = jnp.maximum(rate - (7.0 - y if north else y), 0.0) / rate

        def body(z):
            rows = pl.ds(pl.multiple_of(z * 8, 8), 8)
            for f, (_, _, k) in enumerate(fields[:3]):
                val = own[f, z, at, :]
                own[f, z, at, :] = val + weight * (bs[k, rows, :] - val)

        each(levels, 6, body)

    on_sides(blend)

    parts = [halo_r[0:8, :]]
    parts += [coef[8 * b : 8 * b + 8, :] for b in range(blocks)]
    parts += [halo_r[8:16, :]]
    t = turned([pltpu.roll(part, 8, 1) for part in parts])
    own_r[...] = t[0:16]
    for msg in (north, south):
        for b in range(3):
            msg[levels, 8 * b : 8 * b + 8, :] = zero
    north[levels, 0:HALO, :] = t[2:8]
    south[levels, 0:HALO, :] = t[8:14]


def prep_kernel(
    px, ux, vx, coef, halo_r, width, from_w, from_e, sn_w, sng, sn_e,
    pb, ub, vb, E_, M_,
    bs, bt, rate_, R_,
):
    levels, _, _ = px.shape
    blocks = width.shape[0] // 8
    starts = [OFF - 8 + 8 * b for b in range(blocks + 2)]
    fields = ((px, pb, 2), (ux, ub, 0), (vx, vb, 1))

    def take(z):
        for src, dst, _ in fields:
            for s in starts:
                dst[z, s : s + 8, :] = src[z, s : s + 8, :]

    each(levels, 2, take)

    def blend(north):
        side_bands(sn_w, sng, sn_e, bs, 3 * north)
        for k in range(3):
            for g in range(4):
                bt[k, g] = bs[k, g * LANES : (g + 1) * LANES, :].T
        fill_rates(rate_, width, from_w, from_e)
        y = iota8(1).astype(jnp.float32)
        dist = 127.0 - y if north else y
        for first in range(0, blocks + 2, SB):
            some = range(first, min(first + SB, blocks + 2))
            weights = []
            for b in some:
                rate = jnp.maximum(rate_[8 * b : 8 * b + 8, :], 1.0)
                weights.append(jnp.maximum(rate - dist, 0.0) / rate)

            def trip(g, _):
                for _, dst, k in fields:
                    for i in range(ZS):
                        z = g * ZS + i
                        shift = lax.rem(LANES + 120 * north - 8 * lax.rem(z, 16), LANES)
                        for b, weight in zip(some, weights):
                            s = starts[b]
                            band = pltpu.roll(bt[k, z // 16, s : s + 8, :], shift, 1)
                            val = dst[z, s : s + 8, :]
                            dst[z, s : s + 8, :] = val + weight * (band - val)
                return 0

            lax.fori_loop(0, levels // ZS, trip, 0)

    on_sides(blend)
    lane0 = iota8(1) == 0

    def diverge(z):
        for s in starts:
            u = ub[z, s : s + 8, :]
            u_w = ub[z, s - 1 : s + 7, :]
            v = vb[z, s : s + 8, :]
            v_s = jnp.where(lane0, 0.0, pltpu.roll(v, 1, 1))
            E_[z, s : s + 8, :] = SPREAD * ((u - u_w) + (v - v_s))

    each(levels, 6, diverge)
    fill_coefs(R_, coef, halo_r)
    factors(R_, M_, starts)


def step_kernel(
    p0, u0, v0, w0, e0, M_, coef, halo_r, own, own_r, from_s, from_n,
    u_out, v_out, w_out, p_out,
    P_, E_, W_, S_, Q_, D_, R_, sP, sE, sW, sQ, sM, sR, rows, T_, sems,
):
    levels, size_x, _ = u_out.shape
    blocks = size_x // 8
    starts = [8 * b for b in range(1, blocks + 3)]
    main = [OFF + 8 * b for b in range(blocks)]
    ahead = starts[::2]
    sstarts = [SROW, SROW + 8, NROW, NROW + 8]
    zero = jnp.zeros((8, LANES), jnp.float32)
    sub = iota8(0)
    lane = iota8(1)
    is_west, is_east = axis_ends("gx")
    is_south, is_north = axis_ends("gy")
    mask_w = (sub == 0) & is_west
    mask_e = (sub == 7) & is_east
    smask_w = (lane == OFF) & is_west
    smask_e = (lane == OFF + size_x - 1) & is_east
    smask_s = (sub == 0) & is_south
    smask_n = (sub == 7) & is_north
    lane0 = lane == 0
    lane127 = lane == LANES - 1
    AB = ACCEL * SPREAD

    def unpack(z):
        for f, dst in enumerate((sP, sQ, sM, sW)):
            lo = HALO * f
            dst[z, SROW + 8 : SROW + 16, :] = own[f, z, 8:16, :]
            dst[z, NROW : NROW + 8, :] = own[f, z, 0:8, :]
            dst[z, SROW + 8 - HALO : SROW + 8, :] = from_s[z, lo : lo + HALO, :]
            dst[z, NROW + 8 : NROW + 8 + HALO, :] = from_n[z, lo : lo + HALO, :]

    each(levels, 2, unpack)
    fill_coefs(R_, coef, halo_r)
    sR[SROW + 8 : SROW + 16, :] = own_r[8:16, :]
    sR[NROW : NROW + 8, :] = own_r[0:8, :]
    sR[SROW + 8 - HALO : SROW + 8, :] = from_s[levels, 0:HALO, :]
    sR[NROW + 8 : NROW + 8 + HALO, :] = from_n[levels, 0:HALO, :]

    def strip_init(z):
        for s in sstarts:
            u = sQ[z, s : s + 8, :]
            v = sM[z, s : s + 8, :]
            v_s = sM[z, s - 1 : s + 7, :]
            sE[z, s : s + 8, :] = SPREAD * ((u - pltpu.roll(u, 1, 1)) + (v - v_s))
        rows[SUBSTEPS, pl.ds(2 * z, 1), :] = sM[z, SROW + 7 : SROW + 8, :]

    each(levels, 6, strip_init)

    factors(sR, sM, sstarts)

    def descend(qq, ww, mm, rr, at, sectioned, size, old=None):
        given = ww if old is None else old

        def down(z, qs, ds, last=False):
            new = []
            qn = None if last else [qq[z + 1, s : s + 8, :] for s in at]
            for i, s in enumerate(at):
                rhs = given[z, s : s + 8, :] + (qs[i] if last else qs[i] - qn[i])
                if ds is not None:
                    rhs = rhs + rr[s : s + 8, :] * ds[i]
                d = mm[z, s : s + 8, :] * rhs
                ww[z, s : s + 8, :] = d
                new.append(d)
            return qn, tuple(new)

        groups = levels // size
        for i in range(2 * size):
            sectioned(i)
        qs = [qq[0, s : s + 8, :] for s in at]
        ds = None
        for i in range(size - 1):
            qs, ds = down(i, qs, ds)

        def fwd(g, ds):
            qs = [qq[g * size - 1, s : s + 8, :] for s in at]
            for i in range(size):
                qs, ds = down(g * size - 1 + i, qs, ds)
            for i in range(size):
                sectioned((g + 1) * size + i)
            return ds

        ds = lax.fori_loop(1, groups - 1, fwd, ds)
        first = (groups - 1) * size - 1
        qs = [qq[first, s : s + 8, :] for s in at]
        for i in range(size):
            qs, ds = down(first + i, qs, ds)
        return down(levels - 1, qs, ds, last=True)[1]

    def ascend(pp, qq, ww, mm, rr, at, ws, size, scale=1.0, done=None, also=None):
        def up(z, ws):
            new = []
            if also:
                also(z)
            for j, s in enumerate(at):
                w = ww[z, s : s + 8, :] + mm[z, s : s + 8, :] * (rr[s : s + 8, :] * ws[j])
                ww[z, s : s + 8, :] = w if scale == 1.0 else scale * w
                pp[z + 1, s : s + 8, :] = qq[z + 1, s : s + 8, :] - 0.25 * (ws[j] - w)
                new.append(w)
            return tuple(new)

        chunk = levels // 4 if done else levels
        if also:
            also(levels - 1)
        if scale != 1.0:
            for j, s in enumerate(at):
                ww[levels - 1, s : s + 8, :] = scale * ws[j]
        for hi in range(levels, 0, -chunk):
            top = hi - 1
            left = chunk
            if hi == levels:
                for i in range(size - 1):
                    ws = up(levels - 2 - i, ws)
                top = levels - 1 - size
                left = chunk - size

            def bwd(g, ws):
                for i in range(size):
                    ws = up(top - g * size - i, ws)
                return ws

            ws = lax.fori_loop(0, left // size, bwd, ws)
            if hi == chunk:
                for j, s in enumerate(at):
                    pp[0, s : s + 8, :] = qq[0, s : s + 8, :] - 0.25 * ws[j]
            if done:
                done(hi - chunk, hi)

    def strip_step(k, _):
        def sectioned(z):
            for s in sstarts:
                p = sP[z, s : s + 8, :]
                p_s = sP[z, s - 1 : s + 7, :]
                p_n = sP[z, s + 1 : s + 9, :]
                p_w = jnp.where(smask_w, p, pltpu.roll(p, 1, 1))
                p_e = jnp.where(smask_e, 0.0, pltpu.roll(p, LANES - 1, 1))
                if s == SROW + 8:
                    p_s = jnp.where(smask_s, p, p_s)
                if s == NROW:
                    p_n = jnp.where(smask_n, 0.0, p_n)
                e = sE[z, s : s + 8, :] - AB * (((p_w + p_e) + (p_s + p_n)) - 4.0 * p)
                sE[z, s : s + 8, :] = e
                sQ[z, s : s + 8, :] = p - e
            edge_s = jnp.where(is_south, sP[z, SROW + 8 : SROW + 9, :], sP[z, SROW + 7 : SROW + 8, :])
            edge_n = jnp.where(is_north, 0.0, sP[z, NROW + 8 : NROW + 9, :])
            rows[k, pl.ds(2 * z, 1), :] = edge_s
            rows[k, pl.ds(lax.rem(2 * z + LANES - 1, LANES), 1), :] = edge_n

        ws = descend(sQ, sW, sM, sR, sstarts, sectioned, SU)
        ascend(sP, sQ, sW, sM, sR, sstarts, ws, 6)
        return 0

    lax.fori_loop(0, SUBSTEPS, strip_step, 0)

    for k in range(SUBSTEPS + 1):
        T_[k] = rows[k].T

    def edges(k, z, s):
        return pltpu.roll(T_[k, s : s + 8, :], lax.rem(2 * LANES - 2 * z, LANES), 1)

    def main_down(k, first=False):
        def sectioned(z):
            pp = p0 if first else P_
            for s in starts:
                p = pp[z, s : s + 8, :]
                p_w = pp[z, s - 1 : s + 7, :]
                p_e = pp[z, s + 1 : s + 9, :]
                if s == main[0]:
                    p_w = jnp.where(mask_w, p, p_w)
                if s == main[-1]:
                    p_e = jnp.where(mask_e, 0.0, p_e)
                edge = edges(0, z, s) if first else D_[z, s : s + 8, :] if s in ahead else edges(k, z, s)
                p_s = jnp.where(lane0, edge, pltpu.roll(p, 1, 1))
                p_n = jnp.where(lane127, edge, pltpu.roll(p, LANES - 1, 1))
                if first:
                    e = e0[z, s : s + 8, :] - jnp.where(lane0, SPREAD * edges(SUBSTEPS, z, s), 0.0)
                else:
                    e = E_[z, s : s + 8, :]
                e = e - AB * (((p_w + p_e) + (p_s + p_n)) - 4.0 * p)
                E_[z, s : s + 8, :] = e
                if s != starts[0]:
                    S_[z, s : s + 8, :] = p if first else S_[z, s : s + 8, :] + p
                Q_[z, s : s + 8, :] = p - e

        return descend(Q_, W_, M_, R_, starts, sectioned, FU if first else MU, w0 if first else None)

    def main_up(k, ws):
        def also(z):
            for s in ahead:
                D_[z, s : s + 8, :] = edges(k + 1, z, s)

        ascend(P_, Q_, W_, M_, R_, starts, ws, MB, also=also)

    def main_step(k, _):
        main_up(k, main_down(k))
        return 0

    main_up(0, main_down(0, True))
    lax.fori_loop(1, SUBSTEPS - 1, main_step, 0)
    ws = main_down(SUBSTEPS - 1)

    total = T_[0]
    for k in range(1, SUBSTEPS):
        total = total + T_[k]
    T_[0] = total

    chunk = levels // 4
    copies = []

    def send(src, dst, lo, hi):
        at = slice(OFF, OFF + size_x)
        copy = pltpu.make_async_copy(src.at[lo:hi, at, :], dst.at[lo:hi], sems.at[len(copies)])
        copy.start()
        copies.append(copy)

    def finish(z):
        for s in main:
            total = S_[z, s : s + 8, :]
            east = S_[z, s + 1 : s + 9, :]
            if s == main[-1]:
                east = jnp.where(mask_e, 0.0, east)
            north = jnp.where(lane127, edges(0, z, s), pltpu.roll(total, LANES - 1, 1))
            E_[z, s : s + 8, :] = u0[z, s : s + 8, :] - ACCEL * (east - total)
            S_[z, s : s + 8, :] = v0[z, s : s + 8, :] - ACCEL * (north - total)

    for c in range(4):
        each(chunk, chunk if chunk < 5 else 5, lambda i: finish(c * chunk + i))
        send(E_, u_out, c * chunk, (c + 1) * chunk)
        send(S_, v_out, c * chunk, (c + 1) * chunk)

    def done(lo, hi):
        send(W_, w_out, lo, hi)
        send(P_, p_out, lo + 1 if lo else 0, min(hi + 1, levels))

    ascend(P_, Q_, W_, M_, R_, main, ws[1 : 1 + blocks], chunk if chunk < 5 else 5, 0.5, done)
    for copy in copies:
        copy.wait()


def whole(u_wind, v_wind, w_wind, pressure, vert_coef, we_slab, sn_slab, relax_width):
    levels, size_x, _ = pressure.shape
    stay = [pltpu.with_memory_space_constraint(x, pltpu.HBM) for x in (pressure, u_wind, v_wind, w_wind, vert_coef, relax_width)]
    nx = float(size_x * lax.axis_size("gx"))
    f32 = jnp.float32
    block = jax.ShapeDtypeStruct(pressure.shape, f32)
    message = jax.ShapeDtypeStruct((levels + 1, 4 * HALO, LANES), f32)
    ext = size_x + 2 * OFF
    extended = jax.ShapeDtypeStruct((levels, ext, LANES), f32)

    east, west = pl.pallas_call(
        rim_kernel,
        out_shape=(message, message),
        in_specs=[HBM] * 6,
        out_specs=[VMEM] * 2,
        scratch_shapes=[
            pltpu.VMEM((2, 4, levels, 8, LANES), f32),
            pltpu.VMEM((2, 8, LANES), f32),
            pltpu.VMEM((2, 8, LANES), jnp.int32),
            pltpu.SemaphoreType.DMA((2, 6)),
        ],
        compiler_params=pltpu.CompilerParams(vmem_limit_bytes=24 << 20),
        name="rims",
    )(*stay)
    sn_slab, we_slab, east, west = lax.optimization_barrier((sn_slab, we_slab, east, west))
    from_w = passed_along(east, "gx", 1)
    from_e = passed_along(west, "gx", -1)

    sng = to_edges(sn_slab, "gy")
    sng = jnp.transpose(sng, (1, 0, 2, 3)).reshape(8, size_x, LANES)
    sn_w = passed_along(sng[:, size_x - 8 :], "gx", 1)
    sn_e = passed_along(sng[:, :8], "gx", -1)
    weg = to_edges(we_slab, "gx")

    bands = pltpu.VMEM((3, 512, LANES), f32)
    px, ux, vx, wx, halo_r, own, own_r, north, south = pl.pallas_call(
        lambda *refs: strip_kernel(nx, *refs),
        out_shape=(
            extended,
            extended,
            extended,
            extended,
            jax.ShapeDtypeStruct((16, LANES), f32),
            jax.ShapeDtypeStruct((4, levels, 16, LANES), f32),
            jax.ShapeDtypeStruct((16, LANES), f32),
            message,
            message,
        ),
        in_specs=[HBM] * 4 + [VMEM] * 8,
        out_specs=[VMEM] * 9,
        scratch_shapes=[
            bands,
            bands,
            bands,
            pltpu.VMEM((size_x + 16, LANES), f32),
            pltpu.SemaphoreType.DMA((4,)),
        ],
        compiler_params=pltpu.CompilerParams(vmem_limit_bytes=8 << 20),
        name="strips",
    )(*stay[:4], vert_coef, relax_width, weg, sn_w, sng, sn_e, from_w, from_e)
    from_s = passed_along(north, "gy", 1)
    from_n = passed_along(south, "gy", -1)
    pb, ub, vb, e0, m0 = pl.pallas_call(
        prep_kernel,
        out_shape=(extended,) * 5,
        in_specs=[VMEM] * 11,
        out_specs=[VMEM] * 5,
        scratch_shapes=[
            bands,
            pltpu.VMEM((3, 4, LANES, LANES), f32),
            pltpu.VMEM((size_x + 16, LANES), f32),
            pltpu.VMEM((ext, LANES), f32),
        ],
        compiler_params=pltpu.CompilerParams(vmem_limit_bytes=6 << 20),
        cost_estimate=pl.CostEstimate(flops=20_000_000, bytes_accessed=20_000_000, transcendentals=0),
        name="prep",
    )(px, ux, vx, vert_coef, halo_r, relax_width, from_w, from_e, sn_w, sng, sn_e)

    big = pltpu.VMEM((levels, ext, LANES), f32)
    strip = pltpu.VMEM((levels, SROWS, LANES), f32)
    return pl.pallas_call(
        step_kernel,
        out_shape=(block, block, block, block),
        in_specs=[VMEM] * 12,
        out_specs=[HBM] * 4,
        scratch_shapes=[big] * 6
        + [pltpu.VMEM((ext, LANES), f32)]
        + [strip] * 5
        + [
            pltpu.VMEM((SROWS, LANES), f32),
            pltpu.VMEM((SUBSTEPS + 1, LANES, LANES), f32),
            pltpu.VMEM((SUBSTEPS + 1, LANES, LANES), f32),
            pltpu.SemaphoreType.DMA((16,)),
        ],
        compiler_params=pltpu.CompilerParams(vmem_limit_bytes=30 << 20),
        name="substeps",
    )(pb, ub, vb, wx, e0, m0, vert_coef, halo_r, own, own_r, from_s, from_n)


def solution(mesh):
    placed = (
        P(None, "gx", "gy"),
        P(None, "gx", "gy"),
        P(None, "gx", "gy"),
        P(None, "gx", "gy"),
        P("gx", "gy"),
        P(None, None, None, None, ("gy", "gx")),
        P(None, None, None, None, ("gx", "gy")),
        P("gx", "gy"),
    )
    return jax.shard_map(
        whole,
        mesh=mesh,
        in_specs=placed,
        out_specs=(P(None, "gx", "gy"),) * 4,
        check_vma=False,
    )
```
